8 devices in a mesh: rep: 1 (over z), dp: 8 (over x, y, core).
Axes of the slice: x: 2, y: 2, z: 1, core: 2. Of those that a mesh axis runs over, the one named last changes fastest.
Arguments:
- x: bfloat16 [8, 2048, 640], P(('rep', 'dp'))
- dy: bfloat16 [8, 2048, 640], P(('rep', 'dp'))
- w_gate: bfloat16 [2, 640, 4096], P(None, 'dp')
- w_up: bfloat16 [2, 640, 4096], P(None, 'dp')
- w_down: bfloat16 [2, 4096, 640], P(None, 'dp')
Outputs:
- output 1: bfloat16 [8, 2048, 640], P(('rep', 'dp'))
- output 2: bfloat16 [2, 640, 4096], P('rep', 'dp')
- output 3: bfloat16 [2, 640, 4096], P('rep', 'dp')
- output 4: bfloat16 [2, 4096, 640], P('rep', 'dp')
All inputs are finite; a program needn't handle non-finite values.
Results may differ from the reference program's by a relative error of at most 0.018.
Values are sent between devices in bfloat16 or wider.
A program may use at most 2 GiB of HBM per device.

```python
import jax
import jax.numpy as jnp
from jax import lax

SEQUENCES = 8
TOKENS = 2048
D = 640
FF = 4096
LAYERS = 2
NAMES = ("w_gate", "w_up", "w_down")
SHAPES = {"w_gate": (LAYERS, D, FF), "w_up": (LAYERS, D, FF), "w_down": (LAYERS, FF, D)}


def bump(key, n, height):
    away = (jnp.arange(n, dtype=jnp.int32) - jax.random.randint(key, (), 0, n, jnp.int32)) % n
    return jnp.where(away < n // 8, height, 1.0)


def together(key, own, strength):
    shared = jax.random.normal(key, own.shape[1:], jnp.float32)
    return (own + strength * shared) * lax.rsqrt(1 + strength * strength)


def setup_inputs(seed: int = 0, part: int = 0) -> dict:
    kx, kdy, ka, kb, kz, kf, kh, kl, *kw = jax.random.split(jax.random.key(seed), 8 + len(NAMES))
    kx, kdy, ka, kb = (jax.random.fold_in(k, part) for k in (kx, kdy, ka, kb))
    shape = (SEQUENCES, TOKENS, D)
    much_x, much_dy = jax.random.uniform(kz, (2,), jnp.float32, 0.0, 1.0)
    layers = 2.0 ** jax.random.uniform(kl, (LAYERS, 1, 1), jnp.float32, -1.0, 1.0)
    x = together(ka, jax.random.normal(kx, shape, jnp.float32), much_x) * bump(kf, D, 4.0)
    dy = together(kb, jax.random.normal(kdy, shape, jnp.float32), much_dy)
    drawn = {"x": x.astype(jnp.bfloat16), "dy": (dy * (SEQUENCES * TOKENS) ** -0.5).astype(jnp.bfloat16)}
    for key, name in zip(kw, NAMES, strict=True):
        w = jax.random.normal(key, SHAPES[name], jnp.float32) * SHAPES[name][1] ** -0.5
        drawn[name] = (w * {"w_gate": 1.0, "w_up": bump(kh, FF, 4.0), "w_down": layers}[name]).astype(jnp.bfloat16)
    return drawn


def matmul(a, w):
    return jnp.dot(a, w, preferred_element_type=jnp.float32).astype(jnp.bfloat16)


def normed(h):
    wide = h.astype(jnp.float32)
    scale = lax.rsqrt(jnp.mean(wide**2, -1, keepdims=True) + 1e-6)
    return (wide * scale).astype(jnp.bfloat16)


def layer(h, w):
    a = normed(h)
    gate = jnp.dot(a, w["w_gate"], preferred_element_type=jnp.float32)
    up = jnp.dot(a, w["w_up"], preferred_element_type=jnp.float32)
    return h + matmul((jax.nn.silu(gate) * up).astype(jnp.bfloat16), w["w_down"])


def stack(weights, h):
    return lax.scan(lambda h, w: (layer(h, w), None), h, weights)[0]


def reference(x, dy, w_gate, w_up, w_down):
    weights = dict(zip(NAMES, (w_gate, w_up, w_down), strict=True))

    def take(so_far, sequence):
        h, by_y = sequence
        _, back = jax.vjp(stack, weights, h)
        by_weights, by_h = back(by_y)
        return jax.tree.map(lambda total, term: total + term.astype(jnp.float32), so_far, by_weights), by_h

    none_yet = {name: jnp.zeros(w.shape, jnp.float32) for name, w in weights.items()}
    by_weights, by_x = lax.scan(take, none_yet, (x, dy))
    return (by_x, *(by_weights[name].astype(jnp.bfloat16) for name in NAMES))
```

```python
import jax
import jax.numpy as jnp
from jax import lax
from jax.experimental import pallas as pl
from jax.experimental.pallas import tpu as pltpu
from jax.sharding import PartitionSpec as P

N = 8
T, D, FF, LAYERS = 2048, 640, 4096, 2
CH = 4
F = FF // CH
RB = D // N
CB = F // N
HD = D // 2
STEPS = LAYERS * CH
TB = 512
VB = 256

f32, bf16 = jnp.float32, jnp.bfloat16


def dot(a, b):
    return jnp.dot(a, b, preferred_element_type=f32)


def dot_nt(a, b):
    return lax.dot_general(a, b, (((1,), (1,)), ((), ())), preferred_element_type=f32)


def kernel(
    x_hbm, dy_hbm, gu_own, dn_own,
    dx_hbm, outg_hbm, outd_hbm, gu_all, dn_all,
    wg, wu, wd, h, a, at, dy, dyt, z, dg, du, acc,
    owng, ownd, sibg, sibd, recg, recd, sdg, sdd, rdg, rdd,
    sxg, sxd, syg, syd, bxg, bxd, byg, byd, fing, find, og, od,
    ag_send, ag_recv, load_sem, rs_send, rs_recv, out_sem, in_sem, free_sib, free_diag, free_block,
):
    me = lax.axis_index("dp")
    k = me % 2
    cy = (me // 2) % 2
    cx = me // 4
    chip = 2 * cx + cy
    sib = 2 * chip + (1 - k)
    chip_x = 2 * (1 - cx) + cy
    chip_y = 2 * cx + (1 - cy)
    chip_d = 2 * (1 - cx) + (1 - cy)
    xn, yn, dn = 2 * chip_x + k, 2 * chip_y + k, 2 * chip_d + k

    def far(src, dst, ss, rs, to):
        return pltpu.make_async_remote_copy(
            src_ref=src, dst_ref=dst, send_sem=ss, recv_sem=rs, device_id={"dp": to}, device_id_type=pl.DeviceIdType.MESH
        )

    def signal(sem, to):
        pl.semaphore_signal(sem, inc=1, device_id={"dp": to}, device_id_type=pl.DeviceIdType.MESH)

    def own_copies(j):
        for i, to in enumerate((xn, yn, sib)):
            r = (0, 2, 8)[i]
            yield far(gu_own.at[j], gu_all.at[j, me], ag_send.at[2 * i], ag_recv.at[j, r], to)
            yield far(dn_own.at[j], dn_all.at[j, me], ag_send.at[2 * i + 1], ag_recv.at[j, r + 1], to)

    def forward_copies(j):
        top, bot = pl.ds(0, HD), pl.ds(HD, HD)
        yield far(gu_all.at[j, xn, 0], gu_all.at[j, xn, 0], ag_send.at[6], ag_recv.at[j, 4], yn)
        yield far(dn_all.at[j, xn, top], dn_all.at[j, xn, top], ag_send.at[7], ag_recv.at[j, 5], yn)
        yield far(gu_all.at[j, yn, 1], gu_all.at[j, yn, 1], ag_send.at[8], ag_recv.at[j, 6], xn)
        yield far(dn_all.at[j, yn, bot], dn_all.at[j, yn, bot], ag_send.at[9], ag_recv.at[j, 7], xn)
        for i, src in enumerate((xn, yn)):
            yield far(gu_all.at[j, src], gu_all.at[j, src], ag_send.at[10 + 2 * i], ag_recv.at[j, 10 + 2 * i], sib)
            yield far(dn_all.at[j, src], dn_all.at[j, src], ag_send.at[11 + 2 * i], ag_recv.at[j, 11 + 2 * i], sib)

    def last_copies(j):
        yield far(gu_all.at[j, dn], gu_all.at[j, dn], ag_send.at[14], ag_recv.at[j, 14], sib)
        yield far(dn_all.at[j, dn], dn_all.at[j, dn], ag_send.at[15], ag_recv.at[j, 15], sib)

    def arrived(ref, j, r, frm):
        far(ref, ref, ag_send.at[0], ag_recv.at[j, r], frm).wait_recv()

    def gather_own(j):
        @pl.when(j > 0)
        def _():
            for copy in own_copies(j):
                copy.wait_send()

        for copy in own_copies(j):
            copy.start()

    def gather_forward(j):
        arrived(gu_all.at[j, xn], j, 0, xn)
        arrived(dn_all.at[j, xn], j, 1, xn)
        arrived(gu_all.at[j, yn], j, 2, yn)
        arrived(dn_all.at[j, yn], j, 3, yn)

        @pl.when(j > 0)
        def _():
            for copy in forward_copies(j):
                copy.wait_send()

        for copy in forward_copies(j):
            copy.start()

    def gather_last(j):
        top, bot = pl.ds(0, HD), pl.ds(HD, HD)
        arrived(gu_all.at[j, dn, 0], j, 4, yn)
        arrived(dn_all.at[j, dn, top], j, 5, yn)
        arrived(gu_all.at[j, dn, 1], j, 6, xn)
        arrived(dn_all.at[j, dn, bot], j, 7, xn)

        @pl.when(j > 0)
        def _():
            for copy in last_copies(j):
                copy.wait_send()

        for copy in last_copies(j):
            copy.start()

    def gather_done(j):
        for i, c in enumerate((chip, chip_x, chip_y, chip_d)):
            src = 2 * c + (1 - k)
            r = 8 + 2 * i
            arrived(gu_all.at[j, src], j, r, sib)
            arrived(dn_all.at[j, src], j, r + 1, sib)

    def load_weights(j, slot):
        def parts(gu, down, src):
            rows = pl.ds(pl.multiple_of(src * RB, RB), RB)
            cols = pl.ds(pl.multiple_of(src * CB, CB), CB)
            pltpu.make_async_copy(gu.at[0], wg.at[slot, rows], load_sem.at[slot, 0]).start()
            pltpu.make_async_copy(gu.at[1], wu.at[slot, rows], load_sem.at[slot, 1]).start()
            pltpu.make_async_copy(down, wd.at[slot, :, cols], load_sem.at[slot, 2]).start()

        parts(gu_own.at[j], dn_own.at[j], me)
        for i in range(1, N):
            src = (me + i) % N
            parts(gu_all.at[j, src], dn_all.at[j, src], src)

    def weights_loaded(slot):
        for i, w in enumerate((wg, wu, wd)):
            pltpu.make_async_copy(w.at[slot], w.at[slot], load_sem.at[slot, i]).wait()

    def sib_copies():
        return (
            far(sibg, recg, rs_send.at[0], rs_recv.at[0], sib),
            far(sibd, recd, rs_send.at[1], rs_recv.at[1], sib),
        )

    def diag_copies():
        top, bot = pl.ds(0, HD), pl.ds(HD, HD)
        return (
            far(sdg.at[0], rdg.at[0], rs_send.at[2], rs_recv.at[2], xn),
            far(sdd.at[top], rdd.at[top], rs_send.at[3], rs_recv.at[3], xn),
            far(sdg.at[1], rdg.at[1], rs_send.at[4], rs_recv.at[4], yn),
            far(sdd.at[bot], rdd.at[bot], rs_send.at[5], rs_recv.at[5], yn),
        )

    def block_copies():
        return (
            far(sxg, bxg, rs_send.at[6], rs_recv.at[6], xn),
            far(sxd, bxd, rs_send.at[7], rs_recv.at[7], xn),
            far(syg, byg, rs_send.at[8], rs_recv.at[8], yn),
            far(syd, byd, rs_send.at[9], rs_recv.at[9], yn),
        )

    def out_copies(j):
        return (
            pltpu.make_async_copy(og, outg_hbm.at[j], out_sem.at[0]),
            pltpu.make_async_copy(od, outd_hbm.at[j], out_sem.at[1]),
        )

    def scatter_sib(s):
        @pl.when(s > 0)
        def _():
            pl.semaphore_wait(free_sib, 1)

        for copy in sib_copies():
            copy.start()

    def scatter_diag(s):
        @pl.when(s > 0)
        def _():
            for copy in diag_copies():
                copy.wait_send()

        for copy in sib_copies():
            copy.wait_recv()
        for m in range(2):
            fing[m] = owng[m, chip] + recg[m, chip].astype(f32)
            owng[m, chip_x] = owng[m, chip_x] + recg[m, chip_x].astype(f32)
            owng[m, chip_y] = owng[m, chip_y] + recg[m, chip_y].astype(f32)
            sdg[m] = (owng[m, chip_d] + recg[m, chip_d].astype(f32)).astype(bf16)
        find[...] = ownd[chip] + recd[chip].astype(f32)
        ownd[chip_x] = ownd[chip_x] + recd[chip_x].astype(f32)
        ownd[chip_y] = ownd[chip_y] + recd[chip_y].astype(f32)
        sdd[...] = (ownd[chip_d] + recd[chip_d].astype(f32)).astype(bf16)

        @pl.when(s < STEPS - 1)
        def _():
            signal(free_sib, sib)

        @pl.when(s > 0)
        def _():
            for sem in (free_diag.at[0], free_diag.at[1]):
                pl.semaphore_wait(sem, 1)

        for copy in diag_copies():
            copy.start()

    def scatter_block(s):
        @pl.when(s > 0)
        def _():
            for copy in block_copies():
                copy.wait_send()

        for copy in diag_copies():
            copy.wait_recv()
        top, bot = pl.ds(0, HD), pl.ds(HD, HD)
        sxg[0] = owng[0, chip_x].astype(bf16)
        sxg[1] = (owng[1, chip_x] + rdg[1].astype(f32)).astype(bf16)
        sxd[top] = ownd[chip_x, top].astype(bf16)
        sxd[bot] = (ownd[chip_x, bot] + rdd[bot].astype(f32)).astype(bf16)
        syg[0] = (owng[0, chip_y] + rdg[0].astype(f32)).astype(bf16)
        syg[1] = owng[1, chip_y].astype(bf16)
        syd[top] = (ownd[chip_y, top] + rdd[top].astype(f32)).astype(bf16)
        syd[bot] = ownd[chip_y, bot].astype(bf16)

        @pl.when(s < STEPS - 1)
        def _():
            signal(free_diag.at[0], xn)
            signal(free_diag.at[1], yn)

        @pl.when(s > 0)
        def _():
            for sem in (free_block.at[0], free_block.at[1]):
                pl.semaphore_wait(sem, 1)

        for copy in block_copies():
            copy.start()

    def scatter_final(s):
        j = CH * (1 - s // CH) + s % CH

        @pl.when(s > 0)
        def _():
            for copy in out_copies(j):
                copy.wait()

        for copy in block_copies():
            copy.wait_recv()
        for m in range(2):
            og[m] = (fing[m] + bxg[m].astype(f32) + byg[m].astype(f32)).astype(bf16)
        od[...] = (find[...] + bxd[...].astype(f32) + byd[...].astype(f32)).astype(bf16)

        @pl.when(s < STEPS - 1)
        def _():
            signal(free_block.at[0], xn)
            signal(free_block.at[1], yn)

        for copy in out_copies(j):
            copy.start()

    def scale_of(wide):
        return lax.rsqrt(jnp.mean(wide * wide, -1, keepdims=True) + 1e-6)

    def tokens(t, n):
        return pl.ds(pl.multiple_of(t * n, n), n)

    def set_a(rows, wide):
        v = (wide * scale_of(wide)).astype(bf16)
        a[rows, :] = v
        vt = v.T
        for d in range(N):
            at[(d % 2 + k) % 2, d // 2, :, rows] = vt[d * RB : (d + 1) * RB]

    barrier = pltpu.get_barrier_semaphore()
    for to in (sib, xn, yn):
        signal(barrier, to)
    pl.semaphore_wait(barrier, 3)

    gather_own(0)
    load_x = pltpu.make_async_copy(x_hbm, h, in_sem.at[0])
    load_dy = pltpu.make_async_copy(dy_hbm, dy, in_sem.at[1])
    load_x.start()
    load_dy.start()
    load_x.wait()
    load_dy.wait()

    acc[...] = jnp.zeros_like(acc)

    @pl.loop(0, T // VB)
    def _(t):
        rows = tokens(t, VB)
        set_a(rows, h[rows, :].astype(f32))
        dyt[:, rows] = dy[rows, :].T

    gather_forward(0)
    gather_own(1)
    gather_last(0)
    gather_done(0)
    load_weights(0, 0)

    @pl.loop(0, CH)
    def _(c):
        slot = c % 2
        weights_loaded(slot)

        @pl.loop(0, T // TB)
        def _(t):
            rows = tokens(t, TB)
            gate = dot(a[rows, :], wg[slot])
            up = dot(a[rows, :], wu[slot])
            prod = (gate * jax.nn.sigmoid(gate) * up).astype(bf16)
            acc[:, rows] += dot_nt(wd[slot], prod)

            @pl.when(t == 1)
            def _():
                gather_forward(c + 1)
                gather_own(c + 2)

        gather_last(c + 1)
        gather_done(c + 1)
        load_weights(c + 1, (c + 1) % 2)

    @pl.loop(0, T // VB)
    def _(t):
        rows = tokens(t, VB)
        y = acc[:, rows].T.astype(bf16)
        v = (h[rows, :].astype(f32) + y.astype(f32)).astype(bf16)
        h[rows, :] = v
        set_a(rows, v.astype(f32))

    @pl.loop(0, LAYERS)
    def _(li):
        acc[...] = jnp.zeros_like(acc)

        @pl.loop(0, CH)
        def _(c):
            s = li * CH + c
            slot = c % 2
            weights_loaded(slot)

            @pl.loop(0, T // TB)
            def _(t):
                rows = tokens(t, TB)
                gate = dot(a[rows, :], wg[slot])
                up = dot(a[rows, :], wu[slot])
                dz = dot(dy[rows, :], wd[slot]).astype(bf16).astype(f32)
                sig = jax.nn.sigmoid(gate)
                act = gate * sig
                z[rows, :] = (act * up).astype(bf16)
                du[rows, :] = (dz * act).astype(bf16)
                dg[rows, :] = (dz * up * (sig + act * (1.0 - sig))).astype(bf16)

                @pl.when((t == 1) & (s < CH - 1))
                def _():
                    gather_forward(CH + c + 1)

                @pl.when((t == 1) & (s < CH - 2))
                def _():
                    gather_own(CH + c + 2)

            @pl.when(s > 0)
            def _():
                scatter_block(s - 1)
                for copy in sib_copies():
                    copy.wait_send()

            for m, grad in enumerate((dg, du)):

                @pl.loop(0, F // TB)
                def _(n):
                    cols = tokens(n, TB)
                    w = dot(at[...].reshape(D, T), grad[:, cols])
                    owng[m, :, :, cols] = w[:HD].reshape(4, RB, TB)
                    sibg[m, :, :, cols] = w[HD:].reshape(4, RB, TB).astype(bf16)

            @pl.loop(0, F // TB)
            def _(n):
                w = dot(dyt[...], z[:, tokens(n, TB)])
                for i in range(TB // (2 * CB)):
                    lo, hi = w[:, 2 * CB * i : 2 * CB * i + CB], w[:, 2 * CB * i + CB : 2 * CB * (i + 1)]
                    q = n * (TB // (2 * CB)) + i
                    ownd[q] = jnp.where(k == 0, lo, hi)
                    sibd[q] = jnp.where(k == 0, hi, lo).astype(bf16)

            scatter_sib(s)

            @pl.when(s < CH - 1)
            def _():
                gather_last(CH + c + 1)
                gather_done(CH + c + 1)

            @pl.when(s < STEPS - 1)
            def _():
                load_weights((CH + s + 1) % STEPS, (c + 1) % 2)

            @pl.loop(0, T // TB)
            def _(t):
                rows = tokens(t, TB)
                acc[:, rows] += dot_nt(wg[slot], dg[rows, :]) + dot_nt(wu[slot], du[rows, :])

            @pl.when(s > 0)
            def _():
                scatter_final(s - 1)

            scatter_diag(s)

        @pl.loop(0, T // VB)
        def _(t):
            rows = tokens(t, VB)
            da = acc[:, rows].T.astype(bf16).astype(f32)
            wide = h[rows, :].astype(f32)
            scale = scale_of(wide)
            along = jnp.mean(da * wide, -1, keepdims=True)
            dwide = (da * scale - wide * (along * scale * scale * scale)).astype(bf16)
            v = (dy[rows, :].astype(f32) + dwide.astype(f32)).astype(bf16)
            dy[rows, :] = v

        @pl.when(li == 0)
        def _():
            again = pltpu.make_async_copy(x_hbm, h, in_sem.at[0])
            again.start()

            @pl.loop(0, T // VB)
            def _(t):
                rows = tokens(t, VB)
                dyt[:, rows] = dy[rows, :].T

            again.wait()

            @pl.loop(0, T // VB)
            def _(t):
                rows = tokens(t, VB)
                set_a(rows, h[rows, :].astype(f32))

    store_dx = pltpu.make_async_copy(dy, dx_hbm, in_sem.at[1])
    store_dx.start()
    last = STEPS - 1
    scatter_block(last)
    scatter_final(last)
    for copy in sib_copies() + diag_copies() + block_copies():
        copy.wait_send()
    for copy in out_copies(CH - 1):
        copy.wait()
    for copy in (*own_copies(last), *forward_copies(last), *last_copies(last)):
        copy.wait_send()
    store_dx.wait()


def on_device(x, dy, gu_own, dn_own):
    hbm = pl.BlockSpec(memory_space=pl.ANY)
    shapes = (
        jax.ShapeDtypeStruct((T, D), bf16),
        jax.ShapeDtypeStruct((STEPS, 2, RB, F), bf16),
        jax.ShapeDtypeStruct((STEPS, D, CB), bf16),
        jax.ShapeDtypeStruct((STEPS, N, 2, RB, F), bf16),
        jax.ShapeDtypeStruct((STEPS, N, D, CB), bf16),
    )
    act = pltpu.VMEM((T, D), bf16)
    wide = pltpu.VMEM((T, F), bf16)
    block = [pltpu.VMEM((2, RB, F), bf16), pltpu.VMEM((D, CB), bf16)]
    scratch = [
        *[pltpu.VMEM((2, D, F), bf16)] * 3,
        act, act, pltpu.VMEM((2, 4, RB, T), bf16), act, pltpu.VMEM((D, T), bf16),
        wide, wide, wide, pltpu.VMEM((D, T), f32),
        pltpu.VMEM((2, 4, RB, F), f32), pltpu.VMEM((4, D, CB), f32),
        *[pltpu.VMEM((2, 4, RB, F), bf16), pltpu.VMEM((4, D, CB), bf16)] * 2,
        *block * 6,
        pltpu.VMEM((2, RB, F), f32), pltpu.VMEM((D, CB), f32), *block,
        pltpu.SemaphoreType.DMA((16,)),
        pltpu.SemaphoreType.DMA((STEPS, 16)),
        pltpu.SemaphoreType.DMA((2, 3)),
        pltpu.SemaphoreType.DMA((10,)),
        pltpu.SemaphoreType.DMA((10,)),
        pltpu.SemaphoreType.DMA((2,)),
        pltpu.SemaphoreType.DMA((2,)),
        pltpu.SemaphoreType.REGULAR,
        pltpu.SemaphoreType.REGULAR((2,)),
        pltpu.SemaphoreType.REGULAR((2,)),
    ]
    return pl.pallas_call(
        kernel,
        out_shape=shapes,
        in_specs=[hbm] * 4,
        out_specs=[hbm] * 5,
        scratch_shapes=scratch,
        compiler_params=pltpu.CompilerParams(collective_id=0, has_side_effects=True, vmem_limit_bytes=67_000_000),
        name="layers",
    )(x, dy, gu_own, dn_own)[:3]


def solution(mesh):
    def step(x, dy, w_gate, w_up, w_down):
        def cols(w):
            return w.reshape(LAYERS, RB, N, CH, CB).transpose(0, 3, 1, 2, 4).reshape(LAYERS, CH, RB, F)

        gu = jnp.stack((cols(w_gate), cols(w_up)), 2).reshape(STEPS, 2, RB, F)
        down = w_down.reshape(LAYERS, CH, CB, D).transpose(0, 1, 3, 2).reshape(STEPS, D, CB)
        dx, outg, outd = on_device(x[0], dy[0], gu, down)
        outg = outg.reshape(LAYERS, CH, 2, RB, N, CB).transpose(2, 0, 3, 4, 1, 5).reshape(2, LAYERS, RB, FF)
        outd = outd.reshape(LAYERS, CH, D, CB).transpose(0, 1, 3, 2).reshape(LAYERS, CH * CB, D)
        return dx[None], outg[0], outg[1], outd

    act, weight = P(("rep", "dp")), P(None, "dp")
    return jax.shard_map(
        step,
        mesh=mesh,
        in_specs=(act, act, weight, weight, weight),
        out_specs=(act, P("rep", "dp"), P("rep", "dp"), P("rep", "dp")),
        check_vma=False,
    )
```

```python
import jax
import jax.numpy as jnp
from jax import lax
from jax.experimental import pallas as pl
from jax.experimental.pallas import tpu as pltpu
from jax.sharding import PartitionSpec as P

N = 8
T, D, FF, LAYERS = 2048, 640, 4096, 2
CH = 4
F = FF // CH
RB = D // N
CB = F // N
HD = D // 2
STEPS = LAYERS * CH
TB = 512
VB = 256
TILES = T // VB

f32, bf16 = jnp.float32, jnp.bfloat16


def dot(a, b):
    return jnp.dot(a, b, preferred_element_type=f32)


def dot_nt(a, b):
    return lax.dot_general(a, b, (((1,), (1,)), ((), ())), preferred_element_type=f32)


def kernel(
    x_hbm, dy_hbm, wg_hbm, wu_hbm, wd_hbm,
    dx_hbm, outg_hbm, outu_hbm, outd_hbm, gu_all, dn_all, saved_hbm, z_hbm,
    wg, wu, wd, h, a, at, dy, dyt, z, dg, du, acc,
    owng, ownd, sibg, sibd, recg, recd, sdg, sdd, rdg, rdd,
    sxg, sxd, syg, syd, bxg, bxd, byg, byd, fing, find, og, od,
    packed, dn_own, saved,
    ag_send, ag_recv, load_sem, rs_send, rs_recv, out_sem, in_sem, pack_sem, saved_sem, z_sem, free_sib, free_diag, free_block,
):
    me = lax.axis_index("dp")
    k = me % 2
    cy = (me // 2) % 2
    cx = me // 4
    chip = 2 * cx + cy
    sib = 2 * chip + (1 - k)
    chip_x = 2 * (1 - cx) + cy
    chip_y = 2 * cx + (1 - cy)
    chip_d = 2 * (1 - cx) + (1 - cy)
    xn, yn, dn = 2 * chip_x + k, 2 * chip_y + k, 2 * chip_d + k

    def far(src, dst, ss, rs, to):
        return pltpu.make_async_remote_copy(
            src_ref=src, dst_ref=dst, send_sem=ss, recv_sem=rs, device_id={"dp": to}, device_id_type=pl.DeviceIdType.MESH
        )

    def signal(sem, to):
        pl.semaphore_signal(sem, inc=1, device_id={"dp": to}, device_id_type=pl.DeviceIdType.MESH)

    def own_gu(j):
        for i, to in enumerate((xn, yn, sib)):
            yield far(packed.at[j % 2], gu_all.at[j, me], ag_send.at[2 * i], ag_recv.at[j, (0, 2, 8)[i]], to)

    def own_dn(j):
        for i, to in enumerate((xn, yn, sib)):
            yield far(dn_own.at[j], dn_all.at[j, me], ag_send.at[2 * i + 1], ag_recv.at[j, (1, 3, 9)[i]], to)

    def slabs(j):
        layer, c = j // CH, j % CH
        for d in range(N):
            yield layer, pl.ds(pl.multiple_of(CH * CB * d + CB * c, CB), CB), pl.ds(CB * d, CB)

    def pack(j):
        for layer, there, here in slabs(j):
            for m, w in enumerate((wg_hbm, wu_hbm)):
                pltpu.make_async_copy(w.at[layer, :, there], packed.at[j % 2, m, :, here], pack_sem.at[j % 2]).start()

    def forward_copies(j):
        top, bot = pl.ds(0, HD), pl.ds(HD, HD)
        yield far(gu_all.at[j, xn, 0], gu_all.at[j, xn, 0], ag_send.at[6], ag_recv.at[j, 4], yn)
        yield far(dn_all.at[j, xn, top], dn_all.at[j, xn, top], ag_send.at[7], ag_recv.at[j, 5], yn)
        yield far(gu_all.at[j, yn, 1], gu_all.at[j, yn, 1], ag_send.at[8], ag_recv.at[j, 6], xn)
        yield far(dn_all.at[j, yn, bot], dn_all.at[j, yn, bot], ag_send.at[9], ag_recv.at[j, 7], xn)
        for i, src in enumerate((xn, yn)):
            yield far(gu_all.at[j, src], gu_all.at[j, src], ag_send.at[10 + 2 * i], ag_recv.at[j, 10 + 2 * i], sib)
            yield far(dn_all.at[j, src], dn_all.at[j, src], ag_send.at[11 + 2 * i], ag_recv.at[j, 11 + 2 * i], sib)

    def last_copies(j):
        yield far(gu_all.at[j, dn], gu_all.at[j, dn], ag_send.at[14], ag_recv.at[j, 14], sib)
        yield far(dn_all.at[j, dn], dn_all.at[j, dn], ag_send.at[15], ag_recv.at[j, 15], sib)

    def arrived(ref, j, r, frm):
        far(ref, ref, ag_send.at[0], ag_recv.at[j, r], frm).wait_recv()

    def gather_own_dn(j):
        @pl.when(j > 0)
        def _():
            for copy in own_dn(j):
                copy.wait_send()

        for copy in own_dn(j):
            copy.start()

    def gather_own_gu(j):
        pltpu.make_async_copy(packed.at[j % 2], packed.at[j % 2], pack_sem.at[j % 2]).wait()

        @pl.when(j > 0)
        def _():
            for copy in own_gu(j):
                copy.wait_send()

        for copy in own_gu(j):
            copy.start()

        @pl.when((j > 0) & (j < STEPS - 1))
        def _():
            pack(j + 1)

    def gather_forward(j):
        arrived(gu_all.at[j, xn], j, 0, xn)
        arrived(dn_all.at[j, xn], j, 1, xn)
        arrived(gu_all.at[j, yn], j, 2, yn)
        arrived(dn_all.at[j, yn], j, 3, yn)

        @pl.when(j > 0)
        def _():
            for copy in forward_copies(j):
                copy.wait_send()

        for copy in forward_copies(j):
            copy.start()

    def gather_last(j):
        top, bot = pl.ds(0, HD), pl.ds(HD, HD)
        arrived(gu_all.at[j, dn, 0], j, 4, yn)
        arrived(dn_all.at[j, dn, top], j, 5, yn)
        arrived(gu_all.at[j, dn, 1], j, 6, xn)
        arrived(dn_all.at[j, dn, bot], j, 7, xn)

        @pl.when(j > 0)
        def _():
            for copy in last_copies(j):
                copy.wait_send()

        for copy in last_copies(j):
            copy.start()

    def gather_done(j):
        for i, c in enumerate((chip, chip_x, chip_y, chip_d)):
            src = 2 * c + (1 - k)
            r = 8 + 2 * i
            arrived(gu_all.at[j, src], j, r, sib)
            arrived(dn_all.at[j, src], j, r + 1, sib)

    def load_weights(j, slot):
        def rows(src):
            return pl.ds(pl.multiple_of(src * RB, RB), RB)

        def cols(src):
            return pl.ds(pl.multiple_of(src * CB, CB), CB)

        for layer, there, here in slabs(j):
            for m, (w, to) in enumerate(((wg_hbm, wg), (wu_hbm, wu))):
                pltpu.make_async_copy(w.at[layer, :, there], to.at[slot, rows(me), here], load_sem.at[slot, m]).start()
        pltpu.make_async_copy(dn_own.at[j], wd.at[slot, :, cols(me)], load_sem.at[slot, 2]).start()
        for i in range(1, N):
            src = (me + i) % N
            pltpu.make_async_copy(gu_all.at[j, src, 0], wg.at[slot, rows(src)], load_sem.at[slot, 0]).start()
            pltpu.make_async_copy(gu_all.at[j, src, 1], wu.at[slot, rows(src)], load_sem.at[slot, 1]).start()
            pltpu.make_async_copy(dn_all.at[j, src], wd.at[slot, :, cols(src)], load_sem.at[slot, 2]).start()

    def weights_loaded(slot):
        for i, w in enumerate((wg, wu, wd)):
            pltpu.make_async_copy(w.at[slot], w.at[slot], load_sem.at[slot, i]).wait()

    def sib_copies():
        return (
            far(sibg, recg, rs_send.at[0], rs_recv.at[0], sib),
            far(sibd, recd, rs_send.at[1], rs_recv.at[1], sib),
        )

    def diag_copies():
        top, bot = pl.ds(0, HD), pl.ds(HD, HD)
        return (
            far(sdg.at[0], rdg.at[0], rs_send.at[2], rs_recv.at[2], xn),
            far(sdd.at[top], rdd.at[top], rs_send.at[3], rs_recv.at[3], xn),
            far(sdg.at[1], rdg.at[1], rs_send.at[4], rs_recv.at[4], yn),
            far(sdd.at[bot], rdd.at[bot], rs_send.at[5], rs_recv.at[5], yn),
        )

    def block_copies():
        return (
            far(sxg, bxg, rs_send.at[6], rs_recv.at[6], xn),
            far(sxd, bxd, rs_send.at[7], rs_recv.at[7], xn),
            far(syg, byg, rs_send.at[8], rs_recv.at[8], yn),
            far(syd, byd, rs_send.at[9], rs_recv.at[9], yn),
        )

    def store_out(j):
        for layer, there, here in slabs(j):
            for m, out in enumerate((outg_hbm, outu_hbm)):
                pltpu.make_async_copy(og.at[m, :, here], out.at[layer, :, there], out_sem.at[0]).start()
        rows = pl.ds(pl.multiple_of(j % CH * CB, CB), CB)
        pltpu.make_async_copy(od, outd_hbm.at[j // CH, rows], out_sem.at[1]).start()

    def out_stored():
        pltpu.make_async_copy(og, og, out_sem.at[0]).wait()
        pltpu.make_async_copy(od, od, out_sem.at[1]).wait()

    def scatter_sib(s):
        @pl.when(s > 0)
        def _():
            pl.semaphore_wait(free_sib, 1)

        for copy in sib_copies():
            copy.start()

    def scatter_diag(s):
        @pl.when(s > 0)
        def _():
            for copy in diag_copies():
                copy.wait_send()

        for copy in sib_copies():
            copy.wait_recv()
        for m in range(2):
            fing[m] = owng[m, chip] + recg[m, chip].astype(f32)
            owng[m, chip_x] = owng[m, chip_x] + recg[m, chip_x].astype(f32)
            owng[m, chip_y] = owng[m, chip_y] + recg[m, chip_y].astype(f32)
            sdg[m] = (owng[m, chip_d] + recg[m, chip_d].astype(f32)).astype(bf16)
        find[...] = ownd[chip] + recd[chip].astype(f32)
        ownd[chip_x] = ownd[chip_x] + recd[chip_x].astype(f32)
        ownd[chip_y] = ownd[chip_y] + recd[chip_y].astype(f32)
        sdd[...] = (ownd[chip_d] + recd[chip_d].astype(f32)).astype(bf16)

        @pl.when(s < STEPS - 1)
        def _():
            signal(free_sib, sib)

        @pl.when(s > 0)
        def _():
            for sem in (free_diag.at[0], free_diag.at[1]):
                pl.semaphore_wait(sem, 1)

        for copy in diag_copies():
            copy.start()

    def scatter_block(s):
        @pl.when(s > 0)
        def _():
            for copy in block_copies():
                copy.wait_send()

        for copy in diag_copies():
            copy.wait_recv()
        top, bot = pl.ds(0, HD), pl.ds(HD, HD)
        sxg[0] = owng[0, chip_x].astype(bf16)
        sxg[1] = (owng[1, chip_x] + rdg[1].astype(f32)).astype(bf16)
        sxd[top] = ownd[chip_x, top].astype(bf16)
        sxd[bot] = (ownd[chip_x, bot] + rdd[bot].astype(f32)).astype(bf16)
        syg[0] = (owng[0, chip_y] + rdg[0].astype(f32)).astype(bf16)
        syg[1] = owng[1, chip_y].astype(bf16)
        syd[top] = (ownd[chip_y, top] + rdd[top].astype(f32)).astype(bf16)
        syd[bot] = ownd[chip_y, bot].astype(bf16)

        @pl.when(s < STEPS - 1)
        def _():
            signal(free_diag.at[0], xn)
            signal(free_diag.at[1], yn)

        @pl.when(s > 0)
        def _():
            for sem in (free_block.at[0], free_block.at[1]):
                pl.semaphore_wait(sem, 1)

        for copy in block_copies():
            copy.start()

    def scatter_final(s):
        j = CH * (1 - s // CH) + s % CH

        @pl.when(s > 0)
        def _():
            out_stored()

        for copy in block_copies():
            copy.wait_recv()
        for m in range(2):
            og[m] = (fing[m] + bxg[m].astype(f32) + byg[m].astype(f32)).astype(bf16)
        od[...] = (find[...] + bxd[...].astype(f32) + byd[...].astype(f32)).T.astype(bf16)

        @pl.when(s < STEPS - 1)
        def _():
            signal(free_block.at[0], xn)
            signal(free_block.at[1], yn)

        store_out(j)

    def scale_of(wide):
        return lax.rsqrt(jnp.mean(wide * wide, -1, keepdims=True) + 1e-6)

    def tokens(t, n):
        return pl.ds(pl.multiple_of(t * n, n), n)

    def set_a(rows, wide):
        v = (wide * scale_of(wide)).astype(bf16)
        a[rows, :] = v
        vt = v.T
        for d in range(N):
            at[(d % 2 + k) % 2, d // 2, :, rows] = vt[d * RB : (d + 1) * RB]

    def store_saved(c, t):
        return pltpu.make_async_copy(saved.at[t % 2], saved_hbm.at[c, t], saved_sem.at[t % 2])

    def load_saved(n):
        return pltpu.make_async_copy(saved_hbm.at[n // TILES, n % TILES], saved.at[n % 2], saved_sem.at[n % 2])

    pack(0)
    pack(1)
    raw = a.at[pl.ds(0, LAYERS * CH * CB)]
    load_dn = [pltpu.make_async_copy(wd_hbm.at[i], raw.at[pl.ds(i * CH * CB, CH * CB)], in_sem.at[2 + i]) for i in range(LAYERS)]
    load_x = pltpu.make_async_copy(x_hbm.at[0], h, in_sem.at[0])
    load_dy = pltpu.make_async_copy(dy_hbm.at[0], dy, in_sem.at[1])
    for copy in (*load_dn, load_x, load_dy):
        copy.start()
    barrier = pltpu.get_barrier_semaphore()
    for to in (sib, xn, yn):
        signal(barrier, to)
    pl.semaphore_wait(barrier, 3)

    gather_own_gu(0)
    for copy in load_dn:
        copy.wait()

    @pl.loop(0, STEPS)
    def _(j):
        dn_own[j] = a[tokens(j, CB), :].T

    gather_own_dn(0)
    gather_own_dn(1)
    load_x.wait()
    load_dy.wait()
    acc[...] = jnp.zeros_like(acc)

    @pl.loop(0, T // VB)
    def _(t):
        rows = tokens(t, VB)
        set_a(rows, h[rows, :].astype(f32))
        dyt[:, rows] = dy[rows, :].T

    gather_forward(0)
    gather_own_gu(1)
    gather_last(0)
    gather_done(0)
    load_weights(0, 0)

    @pl.loop(0, CH)
    def _(c):
        slot = c % 2
        weights_loaded(slot)

        @pl.when(c > 0)
        def _():
            pltpu.make_async_copy(z, z_hbm.at[c], z_sem).wait()

        @pl.loop(0, TILES)
        def _(t):
            rows = tokens(t, VB)

            @pl.when(c * TILES + t > 1)
            def _():
                store_saved(c, t).wait()

            gate = dot(a[rows, :], wg[slot])
            up = dot(a[rows, :], wu[slot])
            sig = jax.nn.sigmoid(gate)
            act = gate * sig
            z[rows, :] = (act * up).astype(bf16)
            saved[t % 2, 0] = act
            saved[t % 2, 1] = up * (sig + act * (1.0 - sig))
            store_saved(c, t).start()

            @pl.when(t == 1)
            def _():
                gather_own_dn(c + 2)
                gather_forward(c + 1)
                gather_own_gu(c + 2)

        pltpu.make_async_copy(z, z_hbm.at[c], z_sem).start()

        @pl.loop(0, T // TB)
        def _(t):
            rows = tokens(t, TB)
            acc[:, rows] += dot_nt(wd[slot], z[rows, :])

        gather_last(c + 1)
        gather_done(c + 1)
        load_weights(c + 1, (c + 1) % 2)

    @pl.loop(0, T // VB)
    def _(t):
        rows = tokens(t, VB)
        y = acc[:, rows].T.astype(bf16)
        v = (h[rows, :].astype(f32) + y.astype(f32)).astype(bf16)
        h[rows, :] = v
        set_a(rows, v.astype(f32))

    pltpu.make_async_copy(z, z_hbm.at[CH - 1], z_sem).wait()
    for t in (0, 1):
        store_saved(CH - 1, t).wait()
    for t in (0, 1):
        load_saved(t).start()

    @pl.loop(0, LAYERS)
    def _(li):
        acc[...] = jnp.zeros_like(acc)

        @pl.loop(0, CH)
        def _(c):
            s = li * CH + c
            slot = c % 2
            weights_loaded(slot)

            @pl.when(li == 0)
            def _():
                @pl.loop(0, T // TB)
                def _(t):
                    rows = tokens(t, TB)
                    gate = dot(a[rows, :], wg[slot])
                    up = dot(a[rows, :], wu[slot])
                    dz = dot(dy[rows, :], wd[slot]).astype(bf16).astype(f32)
                    sig = jax.nn.sigmoid(gate)
                    act = gate * sig
                    z[rows, :] = (act * up).astype(bf16)
                    du[rows, :] = (dz * act).astype(bf16)
                    dg[rows, :] = (dz * (up * (sig + act * (1.0 - sig)))).astype(bf16)

                    @pl.when((t == 0) & (s == 0))
                    def _():
                        gather_own_dn(CH + 2)
                        gather_forward(CH + 1)
                        gather_own_gu(CH + 2)

                    @pl.when((t == 0) & (s == 1))
                    def _():
                        gather_last(CH + 2)
                        gather_forward(CH + 3)

            @pl.when(li > 0)
            def _():
                @pl.loop(0, TILES)
                def _(t):
                    rows = tokens(t, VB)
                    n = c * TILES + t
                    dz = dot(dy[rows, :], wd[slot]).astype(bf16).astype(f32)
                    load_saved(n).wait()
                    du[rows, :] = (dz * saved[t % 2, 0]).astype(bf16)
                    dg[rows, :] = (dz * saved[t % 2, 1]).astype(bf16)

                    @pl.when(n < CH * TILES - 2)
                    def _():
                        load_saved(n + 2).start()

            @pl.when(s > 0)
            def _():
                scatter_block(s - 1)
                for copy in sib_copies():
                    copy.wait_send()

            for m, grad in enumerate((dg, du)):

                @pl.loop(0, F // TB)
                def _(n):
                    cols = tokens(n, TB)
                    w = dot(at[...].reshape(D, T), grad[:, cols])
                    owng[m, :, :, cols] = w[:HD].reshape(4, RB, TB)
                    sibg[m, :, :, cols] = w[HD:].reshape(4, RB, TB).astype(bf16)

            @pl.when(li > 0)
            def _():
                pltpu.make_async_copy(z_hbm.at[c], z, z_sem).wait()

            @pl.loop(0, F // TB)
            def _(n):
                w = dot(dyt[...], z[:, tokens(n, TB)])
                for i in range(TB // (2 * CB)):
                    lo, hi = w[:, 2 * CB * i : 2 * CB * i + CB], w[:, 2 * CB * i + CB : 2 * CB * (i + 1)]
                    q = n * (TB // (2 * CB)) + i
                    ownd[q] = jnp.where(k == 0, lo, hi)
                    sibd[q] = jnp.where(k == 0, hi, lo).astype(bf16)

            scatter_sib(s)

            @pl.when((s >= CH - 1) & (s < STEPS - 1))
            def _():
                pltpu.make_async_copy(z_hbm.at[s - (CH - 1)], z, z_sem).start()

            @pl.when(s == 0)
            def _():
                gather_last(CH + 1)
                gather_done(CH + 1)
                gather_own_dn(CH + 3)
                gather_forward(CH + 2)
                gather_own_gu(CH + 3)

            @pl.when(s == 1)
            def _():
                gather_done(CH + 2)
                gather_last(CH + 3)

            @pl.when(s == 2)
            def _():
                gather_done(CH + 3)

            @pl.when(s < STEPS - 1)
            def _():
                load_weights((CH + s + 1) % STEPS, (c + 1) % 2)

            @pl.loop(0, T // TB)
            def _(t):
                rows = tokens(t, TB)
                acc[:, rows] += dot_nt(wg[slot], dg[rows, :]) + dot_nt(wu[slot], du[rows, :])

                @pl.when((t == 2) & (s > 0))
                def _():
                    scatter_final(s - 1)

                @pl.when(t == 2)
                def _():
                    scatter_diag(s)

        @pl.loop(0, T // VB)
        def _(t):
            rows = tokens(t, VB)
            da = acc[:, rows].T.astype(bf16).astype(f32)
            wide = h[rows, :].astype(f32)
            scale = scale_of(wide)
            along = jnp.mean(da * wide, -1, keepdims=True)
            dwide = (da * scale - wide * (along * scale * scale * scale)).astype(bf16)
            v = (dy[rows, :].astype(f32) + dwide.astype(f32)).astype(bf16)
            dy[rows, :] = v
            dyt[:, rows] = v.T

            @pl.when((li > 0) & (t == 3))
            def _():
                scatter_block(STEPS - 1)

        @pl.when(li == 0)
        def _():
            again = pltpu.make_async_copy(x_hbm.at[0], h, in_sem.at[0])
            again.start()
            again.wait()

            @pl.loop(0, T // VB)
            def _(t):
                rows = tokens(t, VB)
                set_a(rows, h[rows, :].astype(f32))

    store_dx = pltpu.make_async_copy(dy, dx_hbm.at[0], in_sem.at[1])
    store_dx.start()
    last = STEPS - 1
    scatter_final(last)
    for copy in sib_copies() + diag_copies() + block_copies():
        copy.wait_send()
    out_stored()
    for copy in (*own_gu(last), *own_dn(last), *forward_copies(last), *last_copies(last)):
        copy.wait_send()
    store_dx.wait()


def on_device(x, dy, w_gate, w_up, w_down):
    hbm = pl.BlockSpec(memory_space=pl.ANY)
    shapes = (
        jax.ShapeDtypeStruct((1, T, D), bf16),
        jax.ShapeDtypeStruct((LAYERS, RB, FF), bf16),
        jax.ShapeDtypeStruct((LAYERS, RB, FF), bf16),
        jax.ShapeDtypeStruct((LAYERS, CH * CB, D), bf16),
        jax.ShapeDtypeStruct((STEPS, N, 2, RB, F), bf16),
        jax.ShapeDtypeStruct((STEPS, N, D, CB), bf16),
        jax.ShapeDtypeStruct((CH, TILES, 2, VB, F), f32),
        jax.ShapeDtypeStruct((CH, T, F), bf16),
    )
    act = pltpu.VMEM((T, D), bf16)
    wide = pltpu.VMEM((T, F), bf16)
    gu, down = pltpu.VMEM((2, RB, F), bf16), pltpu.VMEM((D, CB), bf16)
    dma = pltpu.SemaphoreType.DMA
    scratch = [
        *[pltpu.VMEM((2, D, F), bf16)] * 3,
        act, act, pltpu.VMEM((2, 4, RB, T), bf16), act, pltpu.VMEM((D, T), bf16),
        wide, wide, wide, pltpu.VMEM((D, T), f32),
        pltpu.VMEM((2, 4, RB, F), f32), pltpu.VMEM((4, D, CB), f32),
        *[pltpu.VMEM((2, 4, RB, F), bf16), pltpu.VMEM((4, D, CB), bf16)] * 2,
        *[gu, down] * 6,
        pltpu.VMEM((2, RB, F), f32), pltpu.VMEM((D, CB), f32), gu, pltpu.VMEM((CB, D), bf16),
        pltpu.VMEM((2, 2, RB, F), bf16), pltpu.VMEM((STEPS, D, CB), bf16), pltpu.VMEM((2, 2, VB, F), f32),
        dma((16,)), dma((STEPS, 16)), dma((2, 3)), dma((10,)), dma((10,)), dma((2,)), dma((4,)), dma((2,)), dma((2,)), dma,
        pltpu.SemaphoreType.REGULAR, pltpu.SemaphoreType.REGULAR((2,)), pltpu.SemaphoreType.REGULAR((2,)),
    ]
    return pl.pallas_call(
        kernel,
        out_shape=shapes,
        in_specs=[hbm] * 5,
        out_specs=[hbm] * 8,
        scratch_shapes=scratch,
        compiler_params=pltpu.CompilerParams(collective_id=0, has_side_effects=True, vmem_limit_bytes=67_000_000),
        name="layers",
    )(x, dy, w_gate, w_up, w_down)[:4]


def solution(mesh):
    act, weight = P(("rep", "dp")), P(None, "dp")
    grad = P("rep", "dp")
    return jax.shard_map(
        on_device,
        mesh=mesh,
        in_specs=(act, act, weight, weight, weight),
        out_specs=(act, grad, grad, grad),
        check_vma=False,
    )
```

```python
import jax
import jax.numpy as jnp
from jax import lax
from jax.experimental import pallas as pl
from jax.experimental.pallas import tpu as pltpu
from jax.sharding import PartitionSpec as P

N = 8
T, D, FF, LAYERS = 2048, 640, 4096, 2
CH = 4
F = FF // CH
RB = D // N
CB = F // N
HD = D // 2
STEPS = LAYERS * CH
TB = 512
VB = 256
TILES = T // VB

f32, bf16 = jnp.float32, jnp.bfloat16


def dot(a, b):
    return jnp.dot(a, b, preferred_element_type=f32)


def dot_nt(a, b):
    return lax.dot_general(a, b, (((1,), (1,)), ((), ())), preferred_element_type=f32)


def kernel(
    x_hbm, dy_hbm, wg_hbm, wu_hbm, wd_hbm,
    dx_hbm, outg_hbm, outu_hbm, outd_hbm, gu_all, dn_all, saved_hbm, z_hbm,
    wg, wu, wd, h, a, at, dy, dyt, z, dg, du, acc,
    owng, ownd, sibg, sibd, recg, recd, sdg, sdd, rdg, rdd,
    sxg, sxd, syg, syd, bxg, bxd, byg, byd, fing, find, og, od,
    packed, dn_own, saved,
    ag_send, ag_recv, load_sem, rs_send, rs_recv, out_sem, in_sem, pack_sem, saved_sem, z_sem, free_sib, free_diag, free_block,
):
    me = lax.axis_index("dp")
    k = me % 2
    cy = (me // 2) % 2
    cx = me // 4
    chip = 2 * cx + cy
    sib = 2 * chip + (1 - k)
    chip_x = 2 * (1 - cx) + cy
    chip_y = 2 * cx + (1 - cy)
    chip_d = 2 * (1 - cx) + (1 - cy)
    xn, yn, dn = 2 * chip_x + k, 2 * chip_y + k, 2 * chip_d + k

    def far(src, dst, ss, rs, to):
        return pltpu.make_async_remote_copy(
            src_ref=src, dst_ref=dst, send_sem=ss, recv_sem=rs, device_id={"dp": to}, device_id_type=pl.DeviceIdType.MESH
        )

    def signal(sem, to):
        pl.semaphore_signal(sem, inc=1, device_id={"dp": to}, device_id_type=pl.DeviceIdType.MESH)

    def own_gu(j):
        for i, to in enumerate((xn, yn, sib)):
            yield far(packed.at[j % 2], gu_all.at[j, me], ag_send.at[2 * i], ag_recv.at[j, (0, 2, 8)[i]], to)

    def own_dn(j):
        for i, to in enumerate((xn, yn, sib)):
            yield far(dn_own.at[j], dn_all.at[j, me], ag_send.at[2 * i + 1], ag_recv.at[j, (1, 3, 9)[i]], to)

    def slabs(j):
        layer, c = j // CH, j % CH
        for d in range(N):
            yield layer, pl.ds(pl.multiple_of(CH * CB * d + CB * c, CB), CB), pl.ds(CB * d, CB)

    def pack(j):
        for layer, there, here in slabs(j):
            for m, w in enumerate((wg_hbm, wu_hbm)):
                pltpu.make_async_copy(w.at[layer, :, there], packed.at[j % 2, m, :, here], pack_sem.at[j % 2]).start()

    def forward_gu(j):
        yield far(gu_all.at[j, xn, 0], gu_all.at[j, xn, 0], ag_send.at[6], ag_recv.at[j, 4], yn)
        yield far(gu_all.at[j, yn, 1], gu_all.at[j, yn, 1], ag_send.at[8], ag_recv.at[j, 6], xn)
        for i, src in enumerate((xn, yn)):
            yield far(gu_all.at[j, src], gu_all.at[j, src], ag_send.at[10 + 2 * i], ag_recv.at[j, 10 + 2 * i], sib)

    def forward_dn(j):
        top, bot = pl.ds(0, HD), pl.ds(HD, HD)
        yield far(dn_all.at[j, xn, top], dn_all.at[j, xn, top], ag_send.at[7], ag_recv.at[j, 5], yn)
        yield far(dn_all.at[j, yn, bot], dn_all.at[j, yn, bot], ag_send.at[9], ag_recv.at[j, 7], xn)
        for i, src in enumerate((xn, yn)):
            yield far(dn_all.at[j, src], dn_all.at[j, src], ag_send.at[11 + 2 * i], ag_recv.at[j, 11 + 2 * i], sib)

    def last_copies(j):
        yield far(gu_all.at[j, dn], gu_all.at[j, dn], ag_send.at[14], ag_recv.at[j, 14], sib)
        yield far(dn_all.at[j, dn], dn_all.at[j, dn], ag_send.at[15], ag_recv.at[j, 15], sib)

    def arrived(ref, j, r, frm):
        far(ref, ref, ag_send.at[0], ag_recv.at[j, r], frm).wait_recv()

    def gather_own_dn(j):
        @pl.when(j > 0)
        def _():
            for copy in own_dn(j):
                copy.wait_send()

        for copy in own_dn(j):
            copy.start()

    def gather_own_gu(j):
        pltpu.make_async_copy(packed.at[j % 2], packed.at[j % 2], pack_sem.at[j % 2]).wait()

        @pl.when(j > 0)
        def _():
            for copy in own_gu(j):
                copy.wait_send()

        for copy in own_gu(j):
            copy.start()

        @pl.when((j > 0) & (j < STEPS - 1))
        def _():
            pack(j + 1)

    def gather_forward_gu(j):
        arrived(gu_all.at[j, xn], j, 0, xn)
        arrived(gu_all.at[j, yn], j, 2, yn)

        @pl.when(j > 0)
        def _():
            for copy in forward_gu(j):
                copy.wait_send()

        for copy in forward_gu(j):
            copy.start()

    def gather_forward_dn(j):
        arrived(dn_all.at[j, xn], j, 1, xn)
        arrived(dn_all.at[j, yn], j, 3, yn)

        @pl.when(j > 0)
        def _():
            for copy in forward_dn(j):
                copy.wait_send()

        for copy in forward_dn(j):
            copy.start()

    def gather_forward(j):
        gather_forward_dn(j)
        gather_forward_gu(j)

    def gather_last(j):
        top, bot = pl.ds(0, HD), pl.ds(HD, HD)
        arrived(gu_all.at[j, dn, 0], j, 4, yn)
        arrived(dn_all.at[j, dn, top], j, 5, yn)
        arrived(gu_all.at[j, dn, 1], j, 6, xn)
        arrived(dn_all.at[j, dn, bot], j, 7, xn)

        @pl.when(j > 0)
        def _():
            for copy in last_copies(j):
                copy.wait_send()

        for copy in last_copies(j):
            copy.start()

    def gather_sib(j, which):
        for i in which:
            src = 2 * (chip, chip_x, chip_y, chip_d)[i] + (1 - k)
            arrived(gu_all.at[j, src], j, 8 + 2 * i, sib)
            arrived(dn_all.at[j, src], j, 9 + 2 * i, sib)

    def gather_done(j):
        gather_sib(j, range(4))

    def load_pieces(j, slot, sources, own=False):
        def rows(src):
            return pl.ds(pl.multiple_of(src * RB, RB), RB)

        def cols(src):
            return pl.ds(pl.multiple_of(src * CB, CB), CB)

        for src in sources:
            pltpu.make_async_copy(gu_all.at[j, src, 0], wg.at[slot, rows(src)], load_sem.at[slot, 0]).start()
            pltpu.make_async_copy(gu_all.at[j, src, 1], wu.at[slot, rows(src)], load_sem.at[slot, 1]).start()
            pltpu.make_async_copy(dn_all.at[j, src], wd.at[slot, :, cols(src)], load_sem.at[slot, 2]).start()
        if own:
            for layer, there, here in slabs(j):
                for m, (w, to) in enumerate(((wg_hbm, wg), (wu_hbm, wu))):
                    pltpu.make_async_copy(w.at[layer, :, there], to.at[slot, rows(me), here], load_sem.at[slot, m]).start()
            pltpu.make_async_copy(dn_own.at[j], wd.at[slot, :, cols(me)], load_sem.at[slot, 2]).start()

    def load_weights(j, slot):
        load_pieces(j, slot, [(me + i) % N for i in range(1, N)], own=True)

    def weights_loaded(slot):
        for i, w in enumerate((wg, wu, wd)):
            pltpu.make_async_copy(w.at[slot], w.at[slot], load_sem.at[slot, i]).wait()

    def sib_copies():
        return (
            far(sibg.at[0], recg.at[0], rs_send.at[0], rs_recv.at[0], sib),
            far(sibg.at[1], recg.at[1], rs_send.at[1], rs_recv.at[1], sib),
            far(sibd, recd, rs_send.at[2], rs_recv.at[2], sib),
        )

    def near_copies(which):
        top, bot = pl.ds(0, HD), pl.ds(HD, HD)
        if which == 0:
            return (
                far(sdg.at[0], rdg.at[0], rs_send.at[3], rs_recv.at[3], xn),
                far(sxg.at[0], bxg.at[0], rs_send.at[4], rs_recv.at[4], xn),
            )
        if which == 1:
            return (
                far(sdg.at[1], rdg.at[1], rs_send.at[5], rs_recv.at[5], yn),
                far(syg.at[1], byg.at[1], rs_send.at[6], rs_recv.at[6], yn),
            )
        return (
            far(sdd.at[top], rdd.at[top], rs_send.at[7], rs_recv.at[7], xn),
            far(sdd.at[bot], rdd.at[bot], rs_send.at[8], rs_recv.at[8], yn),
            far(sxd.at[top], bxd.at[top], rs_send.at[9], rs_recv.at[9], xn),
            far(syd.at[bot], byd.at[bot], rs_send.at[10], rs_recv.at[10], yn),
        )

    def sum_copies():
        top, bot = pl.ds(0, HD), pl.ds(HD, HD)
        return (
            far(sxg.at[1], bxg.at[1], rs_send.at[11], rs_recv.at[11], xn),
            far(syg.at[0], byg.at[0], rs_send.at[12], rs_recv.at[12], yn),
            far(sxd.at[bot], bxd.at[bot], rs_send.at[13], rs_recv.at[13], xn),
            far(syd.at[top], byd.at[top], rs_send.at[14], rs_recv.at[14], yn),
        )

    def diag_arrived():
        for copy in (near_copies(0)[0], near_copies(1)[0], *near_copies(2)[:2]):
            copy.wait_recv()

    def blocks_arrived():
        for copy in (near_copies(0)[1], near_copies(1)[1], *near_copies(2)[2:], *sum_copies()):
            copy.wait_recv()

    def store_out(j):
        for layer, there, here in slabs(j):
            for m, out in enumerate((outg_hbm, outu_hbm)):
                pltpu.make_async_copy(og.at[m, :, here], out.at[layer, :, there], out_sem.at[0]).start()
        rows = pl.ds(pl.multiple_of(j % CH * CB, CB), CB)
        pltpu.make_async_copy(od, outd_hbm.at[j // CH, rows], out_sem.at[1]).start()

    def out_stored():
        pltpu.make_async_copy(og, og, out_sem.at[0]).wait()
        pltpu.make_async_copy(od, od, out_sem.at[1]).wait()

    def scatter_sib(s, which):
        if which == 0:
            @pl.when(s > 0)
            def _():
                pl.semaphore_wait(free_sib, 1)

        sib_copies()[which].start()

    def scatter_near(s, which):
        @pl.when(s > 0)
        def _():
            for copy in near_copies(which):
                copy.wait_send()

        sib_copies()[which].wait_recv()
        top, bot = pl.ds(0, HD), pl.ds(HD, HD)
        if which < 2:
            m = which
            fing[m] = owng[m, chip] + recg[m, chip].astype(f32)
            sdg[m] = (owng[m, chip_d] + recg[m, chip_d].astype(f32)).astype(bf16)
            far_x = owng[m, chip_x] + recg[m, chip_x].astype(f32)
            far_y = owng[m, chip_y] + recg[m, chip_y].astype(f32)
            if m == 0:
                sxg[0] = far_x.astype(bf16)
                owng[0, chip_y] = far_y
            else:
                syg[1] = far_y.astype(bf16)
                owng[1, chip_x] = far_x

            @pl.when(s > 0)
            def _():
                pl.semaphore_wait(free_diag.at[m], 1)
                pl.semaphore_wait(free_block.at[m], 1)
        else:
            find[...] = ownd[chip] + recd[chip].astype(f32)
            sdd[...] = (ownd[chip_d] + recd[chip_d].astype(f32)).astype(bf16)
            sxd[top] = (ownd[chip_x, top] + recd[chip_x, top].astype(f32)).astype(bf16)
            ownd[chip_x, bot] = ownd[chip_x, bot] + recd[chip_x, bot].astype(f32)
            syd[bot] = (ownd[chip_y, bot] + recd[chip_y, bot].astype(f32)).astype(bf16)
            ownd[chip_y, top] = ownd[chip_y, top] + recd[chip_y, top].astype(f32)

            @pl.when(s < STEPS - 1)
            def _():
                signal(free_sib, sib)

        for copy in near_copies(which):
            copy.start()

    def scatter_sum(s):
        @pl.when(s > 0)
        def _():
            for copy in sum_copies():
                copy.wait_send()

        diag_arrived()
        top, bot = pl.ds(0, HD), pl.ds(HD, HD)
        sxg[1] = (owng[1, chip_x] + rdg[1].astype(f32)).astype(bf16)
        syg[0] = (owng[0, chip_y] + rdg[0].astype(f32)).astype(bf16)
        sxd[bot] = (ownd[chip_x, bot] + rdd[bot].astype(f32)).astype(bf16)
        syd[top] = (ownd[chip_y, top] + rdd[top].astype(f32)).astype(bf16)

        @pl.when(s < STEPS - 1)
        def _():
            signal(free_diag.at[0], xn)
            signal(free_diag.at[1], yn)

        for copy in sum_copies():
            copy.start()

    def scatter_final(s):
        j = CH * (1 - s // CH) + s % CH

        @pl.when(s > 0)
        def _():
            out_stored()

        blocks_arrived()
        for m in range(2):
            og[m] = (fing[m] + bxg[m].astype(f32) + byg[m].astype(f32)).astype(bf16)
        od[...] = (find[...] + bxd[...].astype(f32) + byd[...].astype(f32)).T.astype(bf16)

        @pl.when(s < STEPS - 1)
        def _():
            signal(free_block.at[0], xn)
            signal(free_block.at[1], yn)

        store_out(j)

    def scale_of(wide):
        return lax.rsqrt(jnp.mean(wide * wide, -1, keepdims=True) + 1e-6)

    def tokens(t, n):
        return pl.ds(pl.multiple_of(t * n, n), n)

    def store_at(rows, v):
        vt = v.T
        for d in range(N):
            at[(d % 2 + k) % 2, d // 2, :, rows] = vt[d * RB : (d + 1) * RB]

    def set_at(rows, wide):
        store_at(rows, (wide * scale_of(wide)).astype(bf16))

    def set_a(rows, wide):
        v = (wide * scale_of(wide)).astype(bf16)
        a[rows, :] = v
        store_at(rows, v)

    def store_saved(c, t):
        return pltpu.make_async_copy(saved.at[t % 2], saved_hbm.at[c, t], saved_sem.at[t % 2])

    def load_saved(n):
        return pltpu.make_async_copy(saved_hbm.at[n // TILES, n % TILES], saved.at[n % 2], saved_sem.at[n % 2])

    pack(0)
    pack(1)
    raw = a.at[pl.ds(0, LAYERS * CH * CB)]
    load_dn = [pltpu.make_async_copy(wd_hbm.at[i], raw.at[pl.ds(i * CH * CB, CH * CB)], in_sem.at[2 + i]) for i in range(LAYERS)]
    load_x = pltpu.make_async_copy(x_hbm.at[0], h, in_sem.at[0])
    load_dy = pltpu.make_async_copy(dy_hbm.at[0], dy, in_sem.at[1])
    for copy in (*load_dn, load_x, load_dy):
        copy.start()
    barrier = pltpu.get_barrier_semaphore()
    for to in (sib, xn, yn):
        signal(barrier, to)
    pl.semaphore_wait(barrier, 3)

    gather_own_gu(0)
    for copy in load_dn:
        copy.wait()

    @pl.loop(0, STEPS)
    def _(j):
        dn_own[j] = a[tokens(j, CB), :].T

    gather_own_dn(0)
    gather_own_dn(1)
    load_x.wait()
    load_dy.wait()
    acc[...] = jnp.zeros_like(acc)

    @pl.loop(0, T // VB)
    def _(t):
        rows = tokens(t, VB)
        set_a(rows, h[rows, :].astype(f32))
        dyt[:, rows] = dy[rows, :].T

    gather_forward_gu(0)
    gather_forward_dn(0)
    gather_own_gu(1)
    gather_last(0)
    gather_done(0)
    load_weights(0, 0)

    @pl.loop(0, CH)
    def _(c):
        slot = c % 2
        weights_loaded(slot)

        @pl.when(c > 0)
        def _():
            pltpu.make_async_copy(z, z_hbm.at[c], z_sem).wait()

        @pl.loop(0, TILES)
        def _(t):
            rows = tokens(t, VB)

            @pl.when(c * TILES + t > 1)
            def _():
                store_saved(c, t).wait()

            gate = dot(a[rows, :], wg[slot])
            up = dot(a[rows, :], wu[slot])
            sig = jax.nn.sigmoid(gate)
            act = gate * sig
            z[rows, :] = (act * up).astype(bf16)
            saved[t % 2, 0] = act
            saved[t % 2, 1] = up * (sig + act * (1.0 - sig))
            store_saved(c, t).start()

            @pl.when(t == 1)
            def _():
                gather_own_dn(c + 2)
                gather_forward(c + 1)
                gather_own_gu(c + 2)
                load_pieces(c + 1, (c + 1) % 2, (xn, yn), own=True)

            @pl.when(t == TILES - 2)
            def _():
                gather_sib(c + 1, range(3))
                load_pieces(c + 1, (c + 1) % 2, [2 * q + (1 - k) for q in (chip, chip_x, chip_y)])

        pltpu.make_async_copy(z, z_hbm.at[c], z_sem).start()

        @pl.loop(0, T // TB)
        def _(t):
            rows = tokens(t, TB)
            acc[:, rows] += dot_nt(wd[slot], z[rows, :])

        gather_last(c + 1)
        load_pieces(c + 1, (c + 1) % 2, (dn,))
        gather_sib(c + 1, (3,))
        load_pieces(c + 1, (c + 1) % 2, (2 * chip_d + (1 - k),))

    @pl.loop(0, T // VB)
    def _(t):
        rows = tokens(t, VB)
        y = acc[:, rows].T.astype(bf16)
        v = (h[rows, :].astype(f32) + y.astype(f32)).astype(bf16)
        h[rows, :] = v
        set_a(rows, v.astype(f32))

    pltpu.make_async_copy(z, z_hbm.at[CH - 1], z_sem).wait()
    for t in (0, 1):
        store_saved(CH - 1, t).wait()
    for t in (0, 1):
        load_saved(t).start()

    @pl.loop(0, LAYERS)
    def _(li):
        acc[...] = jnp.zeros_like(acc)

        @pl.loop(0, CH)
        def _(c):
            s = li * CH + c
            slot = c % 2
            weights_loaded(slot)

            @pl.when(li == 0)
            def _():
                @pl.loop(0, T // TB)
                def _(t):
                    rows = tokens(t, TB)
                    gate = dot(a[rows, :], wg[slot])
                    up = dot(a[rows, :], wu[slot])
                    dz = dot(dy[rows, :], wd[slot]).astype(bf16).astype(f32)
                    sig = jax.nn.sigmoid(gate)
                    act = gate * sig
                    z[rows, :] = (act * up).astype(bf16)
                    du[rows, :] = (dz * act).astype(bf16)
                    dg[rows, :] = (dz * (up * (sig + act * (1.0 - sig)))).astype(bf16)

                    @pl.when((t == 0) & (s == 0))
                    def _():
                        gather_own_dn(CH + 2)
                        gather_forward(CH + 1)
                        gather_own_gu(CH + 2)

                    @pl.when((t == 3) & (s == 0))
                    def _():
                        gather_last(CH + 1)

                    @pl.when((t == 0) & (s > 0) & (s < 3))
                    def _():
                        gather_last(CH + 1 + s)

                    @pl.when((t == 1) & (s > 0))
                    def _():
                        scatter_sum(s - 1)

            @pl.when(li > 0)
            def _():
                @pl.loop(0, TILES)
                def _(t):
                    rows = tokens(t, VB)
                    n = c * TILES + t
                    dz = dot(dy[rows, :], wd[slot]).astype(bf16).astype(f32)
                    load_saved(n).wait()
                    du[rows, :] = (dz * saved[t % 2, 0]).astype(bf16)
                    dg[rows, :] = (dz * saved[t % 2, 1]).astype(bf16)

                    @pl.when(n < CH * TILES - 2)
                    def _():
                        load_saved(n + 2).start()

                    @pl.when(t == 3)
                    def _():
                        scatter_sum(s - 1)

            @pl.when(s > 0)
            def _():
                for copy in sib_copies():
                    copy.wait_send()

            for m, grad in enumerate((dg, du)):

                @pl.loop(0, F // TB)
                def _(n):
                    cols = tokens(n, TB)
                    w = dot(at[...].reshape(D, T), grad[:, cols])
                    owng[m, :, :, cols] = w[:HD].reshape(4, RB, TB)
                    sibg[m, :, :, cols] = w[HD:].reshape(4, RB, TB).astype(bf16)

                scatter_sib(s, m)
                if m == 0:
                    @pl.when(s > 0)
                    def _():
                        scatter_final(s - 1)

            scatter_near(s, 0)

            @pl.when(li > 0)
            def _():
                pltpu.make_async_copy(z_hbm.at[c], z, z_sem).wait()

            @pl.loop(0, F // TB)
            def _(n):
                w = dot(dyt[...], z[:, tokens(n, TB)])
                for i in range(TB // (2 * CB)):
                    lo, hi = w[:, 2 * CB * i : 2 * CB * i + CB], w[:, 2 * CB * i + CB : 2 * CB * (i + 1)]
                    q = n * (TB // (2 * CB)) + i
                    ownd[q] = jnp.where(k == 0, lo, hi)
                    sibd[q] = jnp.where(k == 0, hi, lo).astype(bf16)

            scatter_sib(s, 2)
            scatter_near(s, 1)

            @pl.when(s == CH - 1)
            def _():
                pltpu.make_async_copy(x_hbm.at[0], a, in_sem.at[0]).start()

            @pl.when((s >= CH - 1) & (s < STEPS - 1))
            def _():
                pltpu.make_async_copy(z_hbm.at[s - (CH - 1)], z, z_sem).start()

            @pl.when(s < CH - 1)
            def _():
                gather_done(CH + 1 + s)

            @pl.when(s < STEPS - 1)
            def _():
                load_weights((CH + s + 1) % STEPS, (c + 1) % 2)

            @pl.when(s == 0)
            def _():
                gather_own_dn(CH + 3)
                gather_forward(CH + 2)
                gather_own_gu(CH + 3)

            @pl.when(s == 1)
            def _():
                gather_forward(CH + 3)

            @pl.loop(0, T // TB)
            def _(t):
                rows = tokens(t, TB)
                acc[:, rows] += dot_nt(wg[slot], dg[rows, :]) + dot_nt(wu[slot], du[rows, :])

                @pl.when(t == 1)
                def _():
                    scatter_near(s, 2)

        @pl.when(li == 0)
        def _():
            pltpu.make_async_copy(x_hbm.at[0], a, in_sem.at[0]).wait()

        @pl.loop(0, T // VB)
        def _(t):
            rows = tokens(t, VB)
            da = acc[:, rows].T.astype(bf16).astype(f32)
            wide = h[rows, :].astype(f32)
            scale = scale_of(wide)
            along = jnp.mean(da * wide, -1, keepdims=True)
            dwide = (da * scale - wide * (along * scale * scale * scale)).astype(bf16)
            v = (dy[rows, :].astype(f32) + dwide.astype(f32)).astype(bf16)
            dy[rows, :] = v

            @pl.when(li == 0)
            def _():
                dyt[:, rows] = v.T
                x = a[rows, :]
                h[rows, :] = x
                set_at(rows, x.astype(f32))

            @pl.when(li > 0)
            def _():
                pltpu.make_async_copy(dy.at[rows], dx_hbm.at[0, rows], in_sem.at[1]).start()

                @pl.when(t == 2)
                def _():
                    scatter_sum(STEPS - 1)

    last = STEPS - 1
    scatter_final(last)
    for copy in (*sib_copies(), *near_copies(0), *near_copies(1), *near_copies(2), *sum_copies()):
        copy.wait_send()
    out_stored()
    for copy in (*own_gu(last), *own_dn(last), *forward_gu(last), *forward_dn(last), *last_copies(last)):
        copy.wait_send()
    pltpu.make_async_copy(dy, dx_hbm.at[0], in_sem.at[1]).wait()


def on_device(x, dy, w_gate, w_up, w_down):
    hbm = pl.BlockSpec(memory_space=pl.ANY)
    shapes = (
        jax.ShapeDtypeStruct((1, T, D), bf16),
        jax.ShapeDtypeStruct((LAYERS, RB, FF), bf16),
        jax.ShapeDtypeStruct((LAYERS, RB, FF), bf16),
        jax.ShapeDtypeStruct((LAYERS, CH * CB, D), bf16),
        jax.ShapeDtypeStruct((STEPS, N, 2, RB, F), bf16),
        jax.ShapeDtypeStruct((STEPS, N, D, CB), bf16),
        jax.ShapeDtypeStruct((CH, TILES, 2, VB, F), f32),
        jax.ShapeDtypeStruct((CH, T, F), bf16),
    )
    act = pltpu.VMEM((T, D), bf16)
    wide = pltpu.VMEM((T, F), bf16)
    gu, down = pltpu.VMEM((2, RB, F), bf16), pltpu.VMEM((D, CB), bf16)
    dma = pltpu.SemaphoreType.DMA
    scratch = [
        *[pltpu.VMEM((2, D, F), bf16)] * 3,
        act, act, pltpu.VMEM((2, 4, RB, T), bf16), act, pltpu.VMEM((D, T), bf16),
        wide, wide, wide, pltpu.VMEM((D, T), f32),
        pltpu.VMEM((2, 4, RB, F), f32), pltpu.VMEM((4, D, CB), f32),
        *[pltpu.VMEM((2, 4, RB, F), bf16), pltpu.VMEM((4, D, CB), bf16)] * 2,
        *[gu, down] * 6,
        pltpu.VMEM((2, RB, F), f32), pltpu.VMEM((D, CB), f32), gu, pltpu.VMEM((CB, D), bf16),
        pltpu.VMEM((2, 2, RB, F), bf16), pltpu.VMEM((STEPS, D, CB), bf16), pltpu.VMEM((2, 2, VB, F), f32),
        dma((16,)), dma((STEPS, 16)), dma((2, 3)), dma((15,)), dma((15,)), dma((2,)), dma((4,)), dma((2,)), dma((2,)), dma,
        pltpu.SemaphoreType.REGULAR, pltpu.SemaphoreType.REGULAR((2,)), pltpu.SemaphoreType.REGULAR((2,)),
    ]
    return pl.pallas_call(
        kernel,
        out_shape=shapes,
        in_specs=[hbm] * 5,
        out_specs=[hbm] * 8,
        scratch_shapes=scratch,
        compiler_params=pltpu.CompilerParams(collective_id=0, has_side_effects=True, vmem_limit_bytes=67_000_000),
        name="layers",
    )(x, dy, w_gate, w_up, w_down)[:4]


def solution(mesh):
    act, weight = P(("rep", "dp")), P(None, "dp")
    grad = P("rep", "dp")
    return jax.shard_map(
        on_device,
        mesh=mesh,
        in_specs=(act, act, weight, weight, weight),
        out_specs=(act, grad, grad, grad),
        check_vma=False,
    )
```

```python
import jax
import jax.numpy as jnp
from jax import lax
from jax.experimental import pallas as pl
from jax.experimental.pallas import tpu as pltpu
from jax.sharding import PartitionSpec as P

N = 8
T, D, FF, LAYERS = 2048, 640, 4096, 2
CH = 4
F = FF // CH
RB = D // N
CB = F // N
HD = D // 2
STEPS = LAYERS * CH
TB = 512
VB = 256
WB = 1024
AB = 1024
TILES = T // VB

f32, bf16 = jnp.float32, jnp.bfloat16


def dot(a, b):
    return jnp.dot(a, b, preferred_element_type=f32)


def dot_nt(a, b):
    return lax.dot_general(a, b, (((1,), (1,)), ((), ())), preferred_element_type=f32)


def kernel(
    x_hbm, dy_hbm, wg_hbm, wu_hbm, wd_hbm,
    dx_hbm, outg_hbm, outu_hbm, outd_hbm, gu_all, dn_all, saved_hbm, z_hbm,
    wg, wu, wd, h, a, at, dy, dyt, z, dg, du, acc,
    owng, ownd, sibg, sibd, recg, recd, sdg, sdd, rdg, rdd,
    sxg, sxd, syg, syd, bxg, bxd, byg, byd, fing, find, og, od,
    packed, dn_own, saved,
    ag_send, ag_recv, load_sem, rs_send, rs_recv, out_sem, in_sem, pack_sem, saved_sem, z_sem, free_sib, free_diag, free_block,
):
    me = lax.axis_index("dp")
    k = me % 2
    cy = (me // 2) % 2
    cx = me // 4
    chip = 2 * cx + cy
    sib = 2 * chip + (1 - k)
    chip_x = 2 * (1 - cx) + cy
    chip_y = 2 * cx + (1 - cy)
    chip_d = 2 * (1 - cx) + (1 - cy)
    xn, yn, dn = 2 * chip_x + k, 2 * chip_y + k, 2 * chip_d + k

    def far(src, dst, ss, rs, to):
        return pltpu.make_async_remote_copy(
            src_ref=src, dst_ref=dst, send_sem=ss, recv_sem=rs, device_id={"dp": to}, device_id_type=pl.DeviceIdType.MESH
        )

    def signal(sem, to):
        pl.semaphore_signal(sem, inc=1, device_id={"dp": to}, device_id_type=pl.DeviceIdType.MESH)

    def own_gu(j):
        for i, to in enumerate((xn, yn, sib)):
            yield far(packed.at[j % 2], gu_all.at[j, me], ag_send.at[2 * i], ag_recv.at[j, (0, 2, 8)[i]], to)

    def own_dn(j):
        for i, to in enumerate((xn, yn, sib)):
            yield far(dn_own.at[j], dn_all.at[j, me], ag_send.at[2 * i + 1], ag_recv.at[j, (1, 3, 9)[i]], to)

    def slabs(j):
        layer, c = j // CH, j % CH
        for d in range(N):
            yield layer, pl.ds(pl.multiple_of(CH * CB * d + CB * c, CB), CB), pl.ds(CB * d, CB)

    def pack(j):
        for layer, there, here in slabs(j):
            for m, w in enumerate((wg_hbm, wu_hbm)):
                pltpu.make_async_copy(w.at[layer, :, there], packed.at[j % 2, m, :, here], pack_sem.at[j % 2]).start()

    def forward_gu(j):
        yield far(gu_all.at[j, xn, 0], gu_all.at[j, xn, 0], ag_send.at[6], ag_recv.at[j, 4], yn)
        yield far(gu_all.at[j, yn, 1], gu_all.at[j, yn, 1], ag_send.at[8], ag_recv.at[j, 6], xn)
        for i, src in enumerate((xn, yn)):
            yield far(gu_all.at[j, src], gu_all.at[j, src], ag_send.at[10 + 2 * i], ag_recv.at[j, 10 + 2 * i], sib)

    def forward_dn(j):
        top, bot = pl.ds(0, HD), pl.ds(HD, HD)
        yield far(dn_all.at[j, xn, top], dn_all.at[j, xn, top], ag_send.at[7], ag_recv.at[j, 5], yn)
        yield far(dn_all.at[j, yn, bot], dn_all.at[j, yn, bot], ag_send.at[9], ag_recv.at[j, 7], xn)
        for i, src in enumerate((xn, yn)):
            yield far(dn_all.at[j, src], dn_all.at[j, src], ag_send.at[11 + 2 * i], ag_recv.at[j, 11 + 2 * i], sib)

    def last_copies(j):
        yield far(gu_all.at[j, dn], gu_all.at[j, dn], ag_send.at[14], ag_recv.at[j, 14], sib)
        yield far(dn_all.at[j, dn], dn_all.at[j, dn], ag_send.at[15], ag_recv.at[j, 15], sib)

    def arrived(ref, j, r, frm):
        far(ref, ref, ag_send.at[0], ag_recv.at[j, r], frm).wait_recv()

    def gather_own_dn(j):
        @pl.when(j > 0)
        def _():
            for copy in own_dn(j):
                copy.wait_send()

        for copy in own_dn(j):
            copy.start()

    def gather_own_gu(j):
        pltpu.make_async_copy(packed.at[j % 2], packed.at[j % 2], pack_sem.at[j % 2]).wait()

        @pl.when(j > 0)
        def _():
            for copy in own_gu(j):
                copy.wait_send()

        for copy in own_gu(j):
            copy.start()

        @pl.when((j > 0) & (j < STEPS - 1))
        def _():
            pack(j + 1)

    def gather_forward_gu(j):
        arrived(gu_all.at[j, xn], j, 0, xn)
        arrived(gu_all.at[j, yn], j, 2, yn)

        @pl.when(j > 0)
        def _():
            for copy in forward_gu(j):
                copy.wait_send()

        for copy in forward_gu(j):
            copy.start()

    def gather_forward_dn(j):
        arrived(dn_all.at[j, xn], j, 1, xn)
        arrived(dn_all.at[j, yn], j, 3, yn)

        @pl.when(j > 0)
        def _():
            for copy in forward_dn(j):
                copy.wait_send()

        for copy in forward_dn(j):
            copy.start()

    def gather_forward(j):
        gather_forward_dn(j)
        gather_forward_gu(j)

    def gather_last(j):
        top, bot = pl.ds(0, HD), pl.ds(HD, HD)
        arrived(gu_all.at[j, dn, 0], j, 4, yn)
        arrived(dn_all.at[j, dn, top], j, 5, yn)
        arrived(gu_all.at[j, dn, 1], j, 6, xn)
        arrived(dn_all.at[j, dn, bot], j, 7, xn)

        @pl.when(j > 0)
        def _():
            for copy in last_copies(j):
                copy.wait_send()

        for copy in last_copies(j):
            copy.start()

    def gather_sib(j, which):
        for i in which:
            src = 2 * (chip, chip_x, chip_y, chip_d)[i] + (1 - k)
            arrived(gu_all.at[j, src], j, 8 + 2 * i, sib)
            arrived(dn_all.at[j, src], j, 9 + 2 * i, sib)

    def gather_done(j):
        gather_sib(j, range(4))

    def load_pieces(j, slot, sources, own=False):
        def rows(src):
            return pl.ds(pl.multiple_of(src * RB, RB), RB)

        def cols(src):
            return pl.ds(pl.multiple_of(src * CB, CB), CB)

        for src in sources:
            pltpu.make_async_copy(gu_all.at[j, src, 0], wg.at[slot, rows(src)], load_sem.at[slot, 0]).start()
            pltpu.make_async_copy(gu_all.at[j, src, 1], wu.at[slot, rows(src)], load_sem.at[slot, 1]).start()
            pltpu.make_async_copy(dn_all.at[j, src], wd.at[slot, :, cols(src)], load_sem.at[slot, 2]).start()
        if own:
            for layer, there, here in slabs(j):
                for m, (w, to) in enumerate(((wg_hbm, wg), (wu_hbm, wu))):
                    pltpu.make_async_copy(w.at[layer, :, there], to.at[slot, rows(me), here], load_sem.at[slot, m]).start()
            pltpu.make_async_copy(dn_own.at[j], wd.at[slot, :, cols(me)], load_sem.at[slot, 2]).start()

    def load_weights(j, slot):
        load_pieces(j, slot, [(me + i) % N for i in range(1, N)], own=True)

    def weights_loaded(slot):
        for i, w in enumerate((wg, wu, wd)):
            pltpu.make_async_copy(w.at[slot], w.at[slot], load_sem.at[slot, i]).wait()

    def sib_copies():
        return (
            far(sibg.at[0], recg.at[0], rs_send.at[0], rs_recv.at[0], sib),
            far(sibg.at[1], recg.at[1], rs_send.at[1], rs_recv.at[1], sib),
            far(sibd, recd, rs_send.at[2], rs_recv.at[2], sib),
        )

    def near_copies(which):
        top, bot = pl.ds(0, HD), pl.ds(HD, HD)
        if which == 0:
            return (
                far(sdg.at[0], rdg.at[0], rs_send.at[3], rs_recv.at[3], xn),
                far(sxg.at[0], bxg.at[0], rs_send.at[4], rs_recv.at[4], xn),
            )
        if which == 1:
            return (
                far(sdg.at[1], rdg.at[1], rs_send.at[5], rs_recv.at[5], yn),
                far(syg.at[1], byg.at[1], rs_send.at[6], rs_recv.at[6], yn),
            )
        return (
            far(sdd.at[top], rdd.at[top], rs_send.at[7], rs_recv.at[7], xn),
            far(sdd.at[bot], rdd.at[bot], rs_send.at[8], rs_recv.at[8], yn),
            far(sxd.at[top], bxd.at[top], rs_send.at[9], rs_recv.at[9], xn),
            far(syd.at[bot], byd.at[bot], rs_send.at[10], rs_recv.at[10], yn),
        )

    def sum_copies():
        top, bot = pl.ds(0, HD), pl.ds(HD, HD)
        return (
            far(sxg.at[1], bxg.at[1], rs_send.at[11], rs_recv.at[11], xn),
            far(syg.at[0], byg.at[0], rs_send.at[12], rs_recv.at[12], yn),
            far(sxd.at[bot], bxd.at[bot], rs_send.at[13], rs_recv.at[13], xn),
            far(syd.at[top], byd.at[top], rs_send.at[14], rs_recv.at[14], yn),
        )

    def diag_arrived():
        for copy in (near_copies(0)[0], near_copies(1)[0], *near_copies(2)[:2]):
            copy.wait_recv()

    def blocks_arrived():
        for copy in (near_copies(0)[1], near_copies(1)[1], *near_copies(2)[2:], *sum_copies()):
            copy.wait_recv()

    def store_out(j):
        for layer, there, here in slabs(j):
            for m, out in enumerate((outg_hbm, outu_hbm)):
                pltpu.make_async_copy(og.at[m, :, here], out.at[layer, :, there], out_sem.at[0]).start()
        rows = pl.ds(pl.multiple_of(j % CH * CB, CB), CB)
        pltpu.make_async_copy(od, outd_hbm.at[j // CH, rows], out_sem.at[1]).start()

    def out_stored():
        pltpu.make_async_copy(og, og, out_sem.at[0]).wait()
        pltpu.make_async_copy(od, od, out_sem.at[1]).wait()

    def scatter_sib(s, which):
        if which == 0:
            @pl.when(s > 0)
            def _():
                pl.semaphore_wait(free_sib, 1)

        sib_copies()[which].start()

    def scatter_near(s, which):
        @pl.when(s > 0)
        def _():
            for copy in near_copies(which):
                copy.wait_send()

        sib_copies()[which].wait_recv()
        top, bot = pl.ds(0, HD), pl.ds(HD, HD)
        if which < 2:
            m = which
            fing[m] = owng[m, chip] + recg[m, chip].astype(f32)
            sdg[m] = (owng[m, chip_d] + recg[m, chip_d].astype(f32)).astype(bf16)
            far_x = owng[m, chip_x] + recg[m, chip_x].astype(f32)
            far_y = owng[m, chip_y] + recg[m, chip_y].astype(f32)
            if m == 0:
                sxg[0] = far_x.astype(bf16)
                owng[0, chip_y] = far_y
            else:
                syg[1] = far_y.astype(bf16)
                owng[1, chip_x] = far_x

            @pl.when(s > 0)
            def _():
                pl.semaphore_wait(free_diag.at[m], 1)
                pl.semaphore_wait(free_block.at[m], 1)
        else:
            find[...] = ownd[chip] + recd[chip].astype(f32)
            sdd[...] = (ownd[chip_d] + recd[chip_d].astype(f32)).astype(bf16)
            sxd[top] = (ownd[chip_x, top] + recd[chip_x, top].astype(f32)).astype(bf16)
            ownd[chip_x, bot] = ownd[chip_x, bot] + recd[chip_x, bot].astype(f32)
            syd[bot] = (ownd[chip_y, bot] + recd[chip_y, bot].astype(f32)).astype(bf16)
            ownd[chip_y, top] = ownd[chip_y, top] + recd[chip_y, top].astype(f32)

            @pl.when(s < STEPS - 1)
            def _():
                signal(free_sib, sib)

        for copy in near_copies(which):
            copy.start()

    def scatter_sum(s):
        @pl.when(s > 0)
        def _():
            for copy in sum_copies():
                copy.wait_send()

        diag_arrived()
        top, bot = pl.ds(0, HD), pl.ds(HD, HD)
        sxg[1] = (owng[1, chip_x] + rdg[1].astype(f32)).astype(bf16)
        syg[0] = (owng[0, chip_y] + rdg[0].astype(f32)).astype(bf16)
        sxd[bot] = (ownd[chip_x, bot] + rdd[bot].astype(f32)).astype(bf16)
        syd[top] = (ownd[chip_y, top] + rdd[top].astype(f32)).astype(bf16)

        @pl.when(s < STEPS - 1)
        def _():
            signal(free_diag.at[0], xn)
            signal(free_diag.at[1], yn)

        for copy in sum_copies():
            copy.start()

    def scatter_final(s):
        j = CH * (1 - s // CH) + s % CH

        @pl.when(s > 0)
        def _():
            out_stored()

        blocks_arrived()
        for m in range(2):
            og[m] = (fing[m] + bxg[m].astype(f32) + byg[m].astype(f32)).astype(bf16)
        od[...] = (find[...] + bxd[...].astype(f32) + byd[...].astype(f32)).T.astype(bf16)

        @pl.when(s < STEPS - 1)
        def _():
            signal(free_block.at[0], xn)
            signal(free_block.at[1], yn)

        store_out(j)

    def scale_of(wide):
        return lax.rsqrt(jnp.mean(wide * wide, -1, keepdims=True) + 1e-6)

    def tokens(t, n):
        return pl.ds(pl.multiple_of(t * n, n), n)

    def store_at(rows, v):
        vt = v.T
        for d in range(N):
            at[(d % 2 + k) % 2, d // 2, :, rows] = vt[d * RB : (d + 1) * RB]

    def set_at(rows, wide):
        store_at(rows, (wide * scale_of(wide)).astype(bf16))

    def set_a(rows, wide):
        v = (wide * scale_of(wide)).astype(bf16)
        a[rows, :] = v
        store_at(rows, v)

    def store_saved(c, t):
        return pltpu.make_async_copy(saved.at[t % 2], saved_hbm.at[c, t], saved_sem.at[t % 2])

    def load_saved(n):
        return pltpu.make_async_copy(saved_hbm.at[n // TILES, n % TILES], saved.at[n % 2], saved_sem.at[n % 2])

    pack(0)
    pack(1)
    raw = a.at[pl.ds(0, LAYERS * CH * CB)]
    load_dn = [pltpu.make_async_copy(wd_hbm.at[i], raw.at[pl.ds(i * CH * CB, CH * CB)], in_sem.at[2 + i]) for i in range(LAYERS)]
    load_x = pltpu.make_async_copy(x_hbm.at[0], h, in_sem.at[0])
    load_dy = pltpu.make_async_copy(dy_hbm.at[0], dy, in_sem.at[1])
    for copy in (*load_dn, load_x, load_dy):
        copy.start()
    barrier = pltpu.get_barrier_semaphore()
    for to in (sib, xn, yn):
        signal(barrier, to)
    pl.semaphore_wait(barrier, 3)

    gather_own_gu(0)
    for copy in load_dn:
        copy.wait()

    @pl.loop(0, STEPS)
    def _(j):
        dn_own[j] = a[tokens(j, CB), :].T

    gather_own_dn(0)
    gather_own_dn(1)
    load_x.wait()
    load_dy.wait()
    acc[...] = jnp.zeros_like(acc)

    @pl.loop(0, T // VB)
    def _(t):
        rows = tokens(t, VB)
        set_a(rows, h[rows, :].astype(f32))
        dyt[:, rows] = dy[rows, :].T

    gather_forward_gu(0)
    gather_forward_dn(0)
    gather_own_gu(1)
    gather_own_dn(2)
    gather_last(0)
    gather_done(0)
    load_weights(0, 0)

    @pl.loop(0, CH)
    def _(c):
        slot = c % 2
        weights_loaded(slot)

        @pl.when(c > 0)
        def _():
            pltpu.make_async_copy(z, z_hbm.at[c], z_sem).wait()

        @pl.loop(0, TILES)
        def _(t):
            rows = tokens(t, VB)

            @pl.when(c * TILES + t > 1)
            def _():
                store_saved(c, t).wait()

            gate = dot(a[rows, :], wg[slot])
            up = dot(a[rows, :], wu[slot])
            sig = jax.nn.sigmoid(gate)
            act = gate * sig
            z[rows, :] = (act * up).astype(bf16)
            saved[t % 2, 0] = act
            saved[t % 2, 1] = up * (sig + act * (1.0 - sig))
            store_saved(c, t).start()

            @pl.when(t == 1)
            def _():
                gather_forward(c + 1)
                gather_own_gu(c + 2)
                load_pieces(c + 1, (c + 1) % 2, (xn, yn), own=True)

            @pl.when(t == TILES - 2)
            def _():
                gather_sib(c + 1, range(3))
                load_pieces(c + 1, (c + 1) % 2, [2 * q + (1 - k) for q in (chip, chip_x, chip_y)])

        pltpu.make_async_copy(z, z_hbm.at[c], z_sem).start()

        @pl.loop(0, T // AB)
        def _(t):
            rows = tokens(t, AB)
            acc[:, rows] += dot_nt(wd[slot], z[rows, :])

        gather_last(c + 1)
        gather_own_dn(c + 3)
        load_pieces(c + 1, (c + 1) % 2, (dn,))
        gather_sib(c + 1, (3,))
        load_pieces(c + 1, (c + 1) % 2, (2 * chip_d + (1 - k),))

    @pl.loop(0, T // VB)
    def _(t):
        rows = tokens(t, VB)
        y = acc[:, rows].T.astype(bf16)
        v = (h[rows, :].astype(f32) + y.astype(f32)).astype(bf16)
        h[rows, :] = v
        set_a(rows, v.astype(f32))

    gather_forward(CH + 1)
    gather_own_gu(CH + 2)
    gather_own_dn(CH + 3)

    pltpu.make_async_copy(z, z_hbm.at[CH - 1], z_sem).wait()
    for t in (0, 1):
        store_saved(CH - 1, t).wait()
    for t in (0, 1):
        load_saved(t).start()

    def first_grads(c, t, slot):
        rows = tokens(t, VB)
        n = c * TILES + t
        dz = dot(dy[rows, :], wd[slot]).astype(bf16).astype(f32)
        load_saved(n).wait()
        du[rows, :] = (dz * saved[n % 2, 0]).astype(bf16)
        dg[rows, :] = (dz * saved[n % 2, 1]).astype(bf16)

        @pl.when(n < CH * TILES - 2)
        def _():
            load_saved(n + 2).start()

    @pl.loop(0, LAYERS)
    def _(li):
        acc[...] = jnp.zeros_like(acc)

        @pl.loop(0, CH)
        def _(c):
            s = li * CH + c
            slot = c % 2

            @pl.when((li == 0) | (c == 0))
            def _():
                weights_loaded(slot)

            @pl.when((li > 0) & (c < CH - 1))
            def _():
                load_weights(c + 1, (c + 1) % 2)

            @pl.when(li == 0)
            def _():
                @pl.loop(0, T // TB)
                def _(t):
                    rows = tokens(t, TB)
                    gate = dot(a[rows, :], wg[slot])
                    up = dot(a[rows, :], wu[slot])
                    dz = dot(dy[rows, :], wd[slot]).astype(bf16).astype(f32)
                    sig = jax.nn.sigmoid(gate)
                    act = gate * sig
                    z[rows, :] = (act * up).astype(bf16)
                    du[rows, :] = (dz * act).astype(bf16)
                    dg[rows, :] = (dz * (up * (sig + act * (1.0 - sig)))).astype(bf16)

                    @pl.when((t == 0) & (s == 0))
                    def _():
                        gather_last(CH + 1)

                    @pl.when((t == 3) & (s == 0))
                    def _():
                        gather_forward(CH + 2)
                        gather_own_gu(CH + 3)

                    @pl.when((t == 3) & (s == 2))
                    def _():
                        gather_last(CH + 3)

                    @pl.when((t == 2) & (s > 0))
                    def _():
                        scatter_sum(s - 1)

            @pl.when((li > 0) & (c == 0))
            def _():
                @pl.loop(0, TILES)
                def _(t):
                    first_grads(0, t, 0)

            @pl.when(li > 0)
            def _():
                scatter_sum(s - 1)

            @pl.when(s > 0)
            def _():
                for copy in sib_copies():
                    copy.wait_send()

            for m, grad in enumerate((dg, du)):

                @pl.loop(0, F // WB)
                def _(n):
                    cols = tokens(n, WB)
                    w = dot(at[...].reshape(D, T), grad[:, cols])
                    owng[m, :, :, cols] = w[:HD].reshape(4, RB, WB)
                    sibg[m, :, :, cols] = w[HD:].reshape(4, RB, WB).astype(bf16)

                scatter_sib(s, m)

            @pl.when(s > 0)
            def _():
                scatter_final(s - 1)

            scatter_near(s, 0)

            @pl.when(li > 0)
            def _():
                pltpu.make_async_copy(z_hbm.at[c], z, z_sem).wait()

            @pl.loop(0, F // WB)
            def _(n):
                w = dot(dyt[...], z[:, tokens(n, WB)])
                for i in range(WB // (2 * CB)):
                    lo, hi = w[:, 2 * CB * i : 2 * CB * i + CB], w[:, 2 * CB * i + CB : 2 * CB * (i + 1)]
                    q = n * (WB // (2 * CB)) + i
                    ownd[q] = jnp.where(k == 0, lo, hi)
                    sibd[q] = jnp.where(k == 0, hi, lo).astype(bf16)

            scatter_sib(s, 2)
            scatter_near(s, 1)

            @pl.when(s == CH - 1)
            def _():
                pltpu.make_async_copy(x_hbm.at[0], a, in_sem.at[0]).start()

            @pl.when((s >= CH - 1) & (s < STEPS - 1))
            def _():
                pltpu.make_async_copy(z_hbm.at[s - (CH - 1)], z, z_sem).start()

            @pl.when(s < CH - 1)
            def _():
                gather_done(CH + 1 + s)

            @pl.when(li == 0)
            def _():
                load_weights((CH + s + 1) % STEPS, (c + 1) % 2)

            @pl.when((li > 0) & (c < CH - 1))
            def _():
                weights_loaded((c + 1) % 2)

            @pl.when(s == 1)
            def _():
                gather_forward(CH + 3)

            @pl.loop(0, T // AB)
            def _(t):
                rows = tokens(t, AB)
                acc[:, rows] += dot_nt(wg[slot], dg[rows, :]) + dot_nt(wu[slot], du[rows, :])

                @pl.when((li > 0) & (c < CH - 1))
                def _():
                    for i in range(AB // VB):
                        first_grads(c + 1, t * (AB // VB) + i, (c + 1) % 2)

                @pl.when(t == 0)
                def _():
                    scatter_near(s, 2)

                @pl.when((t == 0) & (s == 0))
                def _():
                    gather_last(CH + 2)

        @pl.when(li == 0)
        def _():
            pltpu.make_async_copy(x_hbm.at[0], a, in_sem.at[0]).wait()

        @pl.loop(0, T // VB)
        def _(t):
            rows = tokens(t, VB)
            da = acc[:, rows].T.astype(bf16).astype(f32)
            wide = h[rows, :].astype(f32)
            scale = scale_of(wide)
            along = jnp.mean(da * wide, -1, keepdims=True)
            dwide = (da * scale - wide * (along * scale * scale * scale)).astype(bf16)
            v = (dy[rows, :].astype(f32) + dwide.astype(f32)).astype(bf16)
            dy[rows, :] = v

            @pl.when(li == 0)
            def _():
                dyt[:, rows] = v.T
                x = a[rows, :]
                h[rows, :] = x
                set_at(rows, x.astype(f32))

            @pl.when(li > 0)
            def _():
                pltpu.make_async_copy(dy.at[rows], dx_hbm.at[0, rows], in_sem.at[1]).start()

                @pl.when(t == 2)
                def _():
                    scatter_sum(STEPS - 1)

    last = STEPS - 1
    scatter_final(last)
    for copy in (*sib_copies(), *near_copies(0), *near_copies(1), *near_copies(2), *sum_copies()):
        copy.wait_send()
    out_stored()
    for copy in (*own_gu(last), *own_dn(last), *forward_gu(last), *forward_dn(last), *last_copies(last)):
        copy.wait_send()
    pltpu.make_async_copy(dy, dx_hbm.at[0], in_sem.at[1]).wait()


def on_device(x, dy, w_gate, w_up, w_down):
    hbm = pl.BlockSpec(memory_space=pl.ANY)
    shapes = (
        jax.ShapeDtypeStruct((1, T, D), bf16),
        jax.ShapeDtypeStruct((LAYERS, RB, FF), bf16),
        jax.ShapeDtypeStruct((LAYERS, RB, FF), bf16),
        jax.ShapeDtypeStruct((LAYERS, CH * CB, D), bf16),
        jax.ShapeDtypeStruct((STEPS, N, 2, RB, F), bf16),
        jax.ShapeDtypeStruct((STEPS, N, D, CB), bf16),
        jax.ShapeDtypeStruct((CH, TILES, 2, VB, F), f32),
        jax.ShapeDtypeStruct((CH, T, F), bf16),
    )
    act = pltpu.VMEM((T, D), bf16)
    wide = pltpu.VMEM((T, F), bf16)
    gu, down = pltpu.VMEM((2, RB, F), bf16), pltpu.VMEM((D, CB), bf16)
    dma = pltpu.SemaphoreType.DMA
    scratch = [
        *[pltpu.VMEM((2, D, F), bf16)] * 3,
        act, act, pltpu.VMEM((2, 4, RB, T), bf16), act, pltpu.VMEM((D, T), bf16),
        wide, wide, wide, pltpu.VMEM((D, T), f32),
        pltpu.VMEM((2, 4, RB, F), f32), pltpu.VMEM((4, D, CB), f32),
        *[pltpu.VMEM((2, 4, RB, F), bf16), pltpu.VMEM((4, D, CB), bf16)] * 2,
        *[gu, down] * 6,
        pltpu.VMEM((2, RB, F), f32), pltpu.VMEM((D, CB), f32), gu, pltpu.VMEM((CB, D), bf16),
        pltpu.VMEM((2, 2, RB, F), bf16), pltpu.VMEM((STEPS, D, CB), bf16), pltpu.VMEM((2, 2, VB, F), f32),
        dma((16,)), dma((STEPS, 16)), dma((2, 3)), dma((15,)), dma((15,)), dma((2,)), dma((4,)), dma((2,)), dma((2,)), dma,
        pltpu.SemaphoreType.REGULAR, pltpu.SemaphoreType.REGULAR((2,)), pltpu.SemaphoreType.REGULAR((2,)),
    ]
    return pl.pallas_call(
        kernel,
        out_shape=shapes,
        in_specs=[hbm] * 5,
        out_specs=[hbm] * 8,
        scratch_shapes=scratch,
        compiler_params=pltpu.CompilerParams(collective_id=0, has_side_effects=True, vmem_limit_bytes=67_000_000),
        name="layers",
    )(x, dy, w_gate, w_up, w_down)[:4]


def solution(mesh):
    act, weight = P(("rep", "dp")), P(None, "dp")
    grad = P("rep", "dp")
    return jax.shard_map(
        on_device,
        mesh=mesh,
        in_specs=(act, act, weight, weight, weight),
        out_specs=(act, grad, grad, grad),
        check_vma=False,
    )
```

```python
import jax
import jax.numpy as jnp
from jax import lax
from jax.experimental import pallas as pl
from jax.experimental.pallas import tpu as pltpu
from jax.sharding import PartitionSpec as P

N = 8
T, D, FF, LAYERS = 2048, 640, 4096, 2
CH = 4
F = FF // CH
RB = D // N
CB = F // N
HD = D // 2
STEPS = LAYERS * CH
TB = 512
VB = 256
WB = 1024
PIECES = 4 + 3 * LAYERS
AB = 1024
TILES = T // VB

f32, bf16 = jnp.float32, jnp.bfloat16


def dot(a, b):
    return jnp.dot(a, b, preferred_element_type=f32)


def dot_nt(a, b):
    return lax.dot_general(a, b, (((1,), (1,)), ((), ())), preferred_element_type=f32)


def kernel(
    x_hbm, dy_hbm, wg_hbm, wu_hbm, wd_hbm,
    dx_hbm, outg_hbm, outu_hbm, outd_hbm, gu_all, dn_all, saved_hbm, z_hbm,
    wg, wu, wd, h, a, at, dy, dyt, z, dg, du, acc,
    owng, ownd, sibg, sibd, recg, recd, sdg, sdd, rdg, rdd,
    sxg, sxd, syg, syd, bxg, bxd, byg, byd, fing, find, og, od,
    packed, dn_own, saved,
    ag_send, ag_recv, load_sem, rs_send, rs_recv, out_sem, in_sem, pack_sem, saved_sem, z_sem, free_sib, free_diag, free_block,
):
    me = lax.axis_index("dp")
    k = me % 2
    cy = (me // 2) % 2
    cx = me // 4
    chip = 2 * cx + cy
    sib = 2 * chip + (1 - k)
    chip_x = 2 * (1 - cx) + cy
    chip_y = 2 * cx + (1 - cy)
    chip_d = 2 * (1 - cx) + (1 - cy)
    xn, yn, dn = 2 * chip_x + k, 2 * chip_y + k, 2 * chip_d + k

    def far(src, dst, ss, rs, to):
        return pltpu.make_async_remote_copy(
            src_ref=src, dst_ref=dst, send_sem=ss, recv_sem=rs, device_id={"dp": to}, device_id_type=pl.DeviceIdType.MESH
        )

    def signal(sem, to):
        pl.semaphore_signal(sem, inc=1, device_id={"dp": to}, device_id_type=pl.DeviceIdType.MESH)

    def own_gu(j):
        for i, to in enumerate((xn, yn, sib)):
            yield far(packed.at[j % 2], gu_all.at[j, me], ag_send.at[2 * i], ag_recv.at[j, (0, 2, 8)[i]], to)

    def own_dn(j):
        for i, to in enumerate((xn, yn, sib)):
            yield far(dn_own.at[j], dn_all.at[j, me], ag_send.at[2 * i + 1], ag_recv.at[j, (1, 3, 9)[i]], to)

    def slabs(j):
        layer, c = j // CH, j % CH
        for d in range(N):
            yield layer, pl.ds(pl.multiple_of(CH * CB * d + CB * c, CB), CB), pl.ds(CB * d, CB)

    def pack(j):
        for layer, there, here in slabs(j):
            for m, w in enumerate((wg_hbm, wu_hbm)):
                pltpu.make_async_copy(w.at[layer, :, there], packed.at[j % 2, m, :, here], pack_sem.at[j % 2]).start()

    def forward_gu(j):
        yield far(gu_all.at[j, xn, 0], gu_all.at[j, xn, 0], ag_send.at[6], ag_recv.at[j, 4], yn)
        yield far(gu_all.at[j, yn, 1], gu_all.at[j, yn, 1], ag_send.at[8], ag_recv.at[j, 6], xn)
        for i, src in enumerate((xn, yn)):
            yield far(gu_all.at[j, src], gu_all.at[j, src], ag_send.at[10 + 2 * i], ag_recv.at[j, 10 + 2 * i], sib)

    def forward_dn(j):
        top, bot = pl.ds(0, HD), pl.ds(HD, HD)
        yield far(dn_all.at[j, xn, top], dn_all.at[j, xn, top], ag_send.at[7], ag_recv.at[j, 5], yn)
        yield far(dn_all.at[j, yn, bot], dn_all.at[j, yn, bot], ag_send.at[9], ag_recv.at[j, 7], xn)
        for i, src in enumerate((xn, yn)):
            yield far(dn_all.at[j, src], dn_all.at[j, src], ag_send.at[11 + 2 * i], ag_recv.at[j, 11 + 2 * i], sib)

    def last_copies(j):
        yield far(gu_all.at[j, dn], gu_all.at[j, dn], ag_send.at[14], ag_recv.at[j, 14], sib)
        yield far(dn_all.at[j, dn], dn_all.at[j, dn], ag_send.at[15], ag_recv.at[j, 15], sib)

    def arrived(ref, j, r, frm):
        far(ref, ref, ag_send.at[0], ag_recv.at[j, r], frm).wait_recv()

    def gather_own_dn(j):
        @pl.when(j > 0)
        def _():
            for copy in own_dn(j):
                copy.wait_send()

        for copy in own_dn(j):
            copy.start()

    def gather_own_gu(j):
        pltpu.make_async_copy(packed.at[j % 2], packed.at[j % 2], pack_sem.at[j % 2]).wait()

        @pl.when(j > 0)
        def _():
            for copy in own_gu(j):
                copy.wait_send()

        for copy in own_gu(j):
            copy.start()

        @pl.when((j > 0) & (j < STEPS - 1))
        def _():
            pack(j + 1)

    def gather_forward_gu(j):
        arrived(gu_all.at[j, xn], j, 0, xn)
        arrived(gu_all.at[j, yn], j, 2, yn)

        @pl.when(j > 0)
        def _():
            for copy in forward_gu(j):
                copy.wait_send()

        for copy in forward_gu(j):
            copy.start()

    def gather_forward_dn(j):
        arrived(dn_all.at[j, xn], j, 1, xn)
        arrived(dn_all.at[j, yn], j, 3, yn)

        @pl.when(j > 0)
        def _():
            for copy in forward_dn(j):
                copy.wait_send()

        for copy in forward_dn(j):
            copy.start()

    def gather_forward(j):
        gather_forward_dn(j)
        gather_forward_gu(j)

    def gather_last(j):
        top, bot = pl.ds(0, HD), pl.ds(HD, HD)
        arrived(gu_all.at[j, dn, 0], j, 4, yn)
        arrived(dn_all.at[j, dn, top], j, 5, yn)
        arrived(gu_all.at[j, dn, 1], j, 6, xn)
        arrived(dn_all.at[j, dn, bot], j, 7, xn)

        @pl.when(j > 0)
        def _():
            for copy in last_copies(j):
                copy.wait_send()

        for copy in last_copies(j):
            copy.start()

    def gather_sib(j, which):
        for i in which:
            src = 2 * (chip, chip_x, chip_y, chip_d)[i] + (1 - k)
            arrived(gu_all.at[j, src], j, 8 + 2 * i, sib)
            arrived(dn_all.at[j, src], j, 9 + 2 * i, sib)

    def gather_done(j):
        gather_sib(j, range(4))

    def load_pieces(j, slot, sources, own=False):
        def rows(src):
            return pl.ds(pl.multiple_of(src * RB, RB), RB)

        def cols(src):
            return pl.ds(pl.multiple_of(src * CB, CB), CB)

        for src in sources:
            pltpu.make_async_copy(gu_all.at[j, src, 0], wg.at[slot, rows(src)], load_sem.at[slot, 0]).start()
            pltpu.make_async_copy(gu_all.at[j, src, 1], wu.at[slot, rows(src)], load_sem.at[slot, 1]).start()
            pltpu.make_async_copy(dn_all.at[j, src], wd.at[slot, :, cols(src)], load_sem.at[slot, 2]).start()
        if own:
            for layer, there, here in slabs(j):
                for m, (w, to) in enumerate(((wg_hbm, wg), (wu_hbm, wu))):
                    pltpu.make_async_copy(w.at[layer, :, there], to.at[slot, rows(me), here], load_sem.at[slot, m]).start()
            pltpu.make_async_copy(dn_own.at[j], wd.at[slot, :, cols(me)], load_sem.at[slot, 2]).start()

    def load_weights(j, slot):
        load_pieces(j, slot, [(me + i) % N for i in range(1, N)], own=True)

    def weights_loaded(slot):
        for i, w in enumerate((wg, wu, wd)):
            pltpu.make_async_copy(w.at[slot], w.at[slot], load_sem.at[slot, i]).wait()

    def sib_copies():
        return (
            far(sibg.at[0], recg.at[0], rs_send.at[0], rs_recv.at[0], sib),
            far(sibg.at[1], recg.at[1], rs_send.at[1], rs_recv.at[1], sib),
            far(sibd, recd, rs_send.at[2], rs_recv.at[2], sib),
        )

    def halves(which):
        if which == 2:
            return lambda g, d: (d.at[pl.ds(0, HD)], d.at[pl.ds(HD, HD)])
        return lambda g, d: (g.at[which, :, pl.ds(0, F // 2)], g.at[which, :, pl.ds(F // 2, F // 2)])

    def near_copies(which):
        of, i = halves(which), 3 + 4 * which
        return (
            far(of(sdg, sdd)[0], of(rdg, rdd)[0], rs_send.at[i], rs_recv.at[i], xn),
            far(of(sdg, sdd)[1], of(rdg, rdd)[1], rs_send.at[i + 1], rs_recv.at[i + 1], yn),
            far(of(sxg, sxd)[0], of(bxg, bxd)[0], rs_send.at[i + 2], rs_recv.at[i + 2], xn),
            far(of(syg, syd)[1], of(byg, byd)[1], rs_send.at[i + 3], rs_recv.at[i + 3], yn),
        )

    def sum_copies():
        copies = []
        for which in range(3):
            of, i = halves(which), 15 + 2 * which
            copies.append(far(of(sxg, sxd)[1], of(bxg, bxd)[1], rs_send.at[i], rs_recv.at[i], xn))
            copies.append(far(of(syg, syd)[0], of(byg, byd)[0], rs_send.at[i + 1], rs_recv.at[i + 1], yn))
        return copies

    def diag_arrived():
        for which in range(3):
            for copy in near_copies(which)[:2]:
                copy.wait_recv()

    def blocks_arrived():
        for which in range(3):
            for copy in near_copies(which)[2:]:
                copy.wait_recv()
        for copy in sum_copies():
            copy.wait_recv()

    def store_out(j):
        for layer, there, here in slabs(j):
            for m, out in enumerate((outg_hbm, outu_hbm)):
                pltpu.make_async_copy(og.at[m, :, here], out.at[layer, :, there], out_sem.at[0]).start()
        rows = pl.ds(pl.multiple_of(j % CH * CB, CB), CB)
        pltpu.make_async_copy(od, outd_hbm.at[j // CH, rows], out_sem.at[1]).start()

    def out_stored():
        pltpu.make_async_copy(og, og, out_sem.at[0]).wait()
        pltpu.make_async_copy(od, od, out_sem.at[1]).wait()

    def scatter_sib(s, which):
        if which == 0:
            @pl.when(s > 0)
            def _():
                pl.semaphore_wait(free_sib, 1)

        sib_copies()[which].start()

    def scatter_near(s, which):
        @pl.when(s > 0)
        def _():
            for copy in near_copies(which):
                copy.wait_send()

        sib_copies()[which].wait_recv()
        top, bot = pl.ds(0, HD), pl.ds(HD, HD)
        if which < 2:
            m = which
            fing[m] = owng[m, chip] + recg[m, chip].astype(f32)
            sdg[m] = (owng[m, chip_d] + recg[m, chip_d].astype(f32)).astype(bf16)
            far_x = owng[m, chip_x] + recg[m, chip_x].astype(f32)
            far_y = owng[m, chip_y] + recg[m, chip_y].astype(f32)
            sxg[m, :, : F // 2] = far_x[:, : F // 2].astype(bf16)
            owng[m, chip_x, :, F // 2 :] = far_x[:, F // 2 :]
            syg[m, :, F // 2 :] = far_y[:, F // 2 :].astype(bf16)
            owng[m, chip_y, :, : F // 2] = far_y[:, : F // 2]

            if m == 0:
                @pl.when(s > 0)
                def _():
                    for sem in (free_diag, free_block):
                        for i in range(2):
                            pl.semaphore_wait(sem.at[i], 1)
        else:
            find[...] = ownd[chip] + recd[chip].astype(f32)
            sdd[...] = (ownd[chip_d] + recd[chip_d].astype(f32)).astype(bf16)
            sxd[top] = (ownd[chip_x, top] + recd[chip_x, top].astype(f32)).astype(bf16)
            ownd[chip_x, bot] = ownd[chip_x, bot] + recd[chip_x, bot].astype(f32)
            syd[bot] = (ownd[chip_y, bot] + recd[chip_y, bot].astype(f32)).astype(bf16)
            ownd[chip_y, top] = ownd[chip_y, top] + recd[chip_y, top].astype(f32)

            @pl.when(s < STEPS - 1)
            def _():
                signal(free_sib, sib)

        for copy in near_copies(which):
            copy.start()

    def scatter_sum(s):
        @pl.when(s > 0)
        def _():
            for copy in sum_copies():
                copy.wait_send()

        diag_arrived()
        top, bot = pl.ds(0, HD), pl.ds(HD, HD)
        lo, hi = pl.ds(0, F // 2), pl.ds(F // 2, F // 2)
        for m in range(2):
            sxg[m, :, hi] = (owng[m, chip_x, :, hi] + rdg[m, :, hi].astype(f32)).astype(bf16)
            syg[m, :, lo] = (owng[m, chip_y, :, lo] + rdg[m, :, lo].astype(f32)).astype(bf16)
        sxd[bot] = (ownd[chip_x, bot] + rdd[bot].astype(f32)).astype(bf16)
        syd[top] = (ownd[chip_y, top] + rdd[top].astype(f32)).astype(bf16)

        @pl.when(s < STEPS - 1)
        def _():
            signal(free_diag.at[0], xn)
            signal(free_diag.at[1], yn)

        for copy in sum_copies():
            copy.start()

    def scatter_final(s):
        j = CH * (1 - s // CH) + s % CH

        @pl.when(s > 0)
        def _():
            out_stored()

        blocks_arrived()
        for m in range(2):
            og[m] = (fing[m] + bxg[m].astype(f32) + byg[m].astype(f32)).astype(bf16)
        od[...] = (find[...] + bxd[...].astype(f32) + byd[...].astype(f32)).T.astype(bf16)

        @pl.when(s < STEPS - 1)
        def _():
            signal(free_block.at[0], xn)
            signal(free_block.at[1], yn)

        store_out(j)

    def scale_of(wide):
        return lax.rsqrt(jnp.mean(wide * wide, -1, keepdims=True) + 1e-6)

    def tokens(t, n):
        return pl.ds(pl.multiple_of(t * n, n), n)

    def store_at(rows, v):
        vt = v.T
        for d in range(N):
            at[(d % 2 + k) % 2, d // 2, :, rows] = vt[d * RB : (d + 1) * RB]

    def set_at(rows, wide):
        store_at(rows, (wide * scale_of(wide)).astype(bf16))

    def set_a(rows, wide):
        v = (wide * scale_of(wide)).astype(bf16)
        a[rows, :] = v
        store_at(rows, v)

    def store_saved(c, t):
        return pltpu.make_async_copy(saved.at[t % 2], saved_hbm.at[c, t], saved_sem.at[t % 2])

    def load_saved(n):
        return pltpu.make_async_copy(saved_hbm.at[n // TILES, n % TILES], saved.at[n % 2], saved_sem.at[n % 2])

    pack(0)
    pack(1)
    raw = a.at[pl.ds(0, LAYERS * CH * CB)]
    load_dn = [pltpu.make_async_copy(wd_hbm.at[i], raw.at[pl.ds(i * CH * CB, CH * CB)], in_sem.at[2 + i]) for i in range(LAYERS)]
    load_x = pltpu.make_async_copy(x_hbm.at[0], h, in_sem.at[0])
    load_dy = pltpu.make_async_copy(dy_hbm.at[0], dy, in_sem.at[1])
    for copy in (*load_dn, load_x, load_dy):
        copy.start()
    barrier = pltpu.get_barrier_semaphore()
    for to in (sib, xn, yn):
        signal(barrier, to)
    pl.semaphore_wait(barrier, 3)

    gather_own_gu(0)
    for copy in load_dn:
        copy.wait()

    @pl.loop(0, STEPS)
    def _(j):
        dn_own[j] = a[tokens(j, CB), :].T

    gather_own_dn(0)
    gather_own_dn(1)
    load_x.wait()
    load_dy.wait()
    acc[...] = jnp.zeros_like(acc)

    @pl.loop(0, T // VB)
    def _(t):
        rows = tokens(t, VB)
        set_a(rows, h[rows, :].astype(f32))
        dyt[:, rows] = dy[rows, :].T

    gather_forward_gu(0)
    gather_forward_dn(0)
    gather_own_gu(1)
    gather_own_dn(2)
    gather_last(0)
    gather_done(0)
    load_weights(0, 0)

    @pl.loop(0, CH)
    def _(c):
        slot = c % 2
        weights_loaded(slot)

        @pl.when(c > 0)
        def _():
            pltpu.make_async_copy(z, z_hbm.at[c], z_sem).wait()

        @pl.loop(0, TILES)
        def _(t):
            rows = tokens(t, VB)

            @pl.when(c * TILES + t > 1)
            def _():
                store_saved(c, t).wait()

            gate = dot(a[rows, :], wg[slot])
            up = dot(a[rows, :], wu[slot])
            sig = jax.nn.sigmoid(gate)
            act = gate * sig
            z[rows, :] = (act * up).astype(bf16)
            saved[t % 2, 0] = act
            saved[t % 2, 1] = up * (sig + act * (1.0 - sig))
            store_saved(c, t).start()

            @pl.when(t == 1)
            def _():
                gather_forward(c + 1)
                gather_own_gu(c + 2)
                load_pieces(c + 1, (c + 1) % 2, (xn, yn), own=True)

            @pl.when(t == TILES - 2)
            def _():
                gather_sib(c + 1, range(3))
                load_pieces(c + 1, (c + 1) % 2, [2 * q + (1 - k) for q in (chip, chip_x, chip_y)])

        pltpu.make_async_copy(z, z_hbm.at[c], z_sem).start()

        @pl.loop(0, T // AB)
        def _(t):
            rows = tokens(t, AB)
            acc[:, rows] += dot_nt(wd[slot], z[rows, :])

        gather_last(c + 1)
        gather_own_dn(c + 3)
        load_pieces(c + 1, (c + 1) % 2, (dn,))

        @pl.when(c < CH - 1)
        def _():
            gather_sib(c + 1, (3,))
            load_pieces(c + 1, (c + 1) % 2, (2 * chip_d + (1 - k),))

    @pl.loop(0, T // VB)
    def _(t):
        rows = tokens(t, VB)
        y = acc[:, rows].T.astype(bf16)
        v = (h[rows, :].astype(f32) + y.astype(f32)).astype(bf16)
        h[rows, :] = v
        set_a(rows, v.astype(f32))

        @pl.when(t == 4)
        def _():
            gather_sib(CH, (3,))
            load_pieces(CH, 0, (2 * chip_d + (1 - k),))

    gather_forward(CH + 1)
    gather_own_gu(CH + 2)
    gather_own_dn(CH + 3)

    pltpu.make_async_copy(z, z_hbm.at[CH - 1], z_sem).wait()
    for t in (0, 1):
        store_saved(CH - 1, t).wait()
    for t in (0, 1):
        load_saved(t).start()

    def first_grads(c, t, slot):
        rows = tokens(t, VB)
        n = c * TILES + t
        dz = dot(dy[rows, :], wd[slot]).astype(bf16).astype(f32)
        load_saved(n).wait()
        du[rows, :] = (dz * saved[n % 2, 0]).astype(bf16)
        dg[rows, :] = (dz * saved[n % 2, 1]).astype(bf16)

        @pl.when(n < CH * TILES - 2)
        def _():
            load_saved(n + 2).start()

    @pl.loop(0, LAYERS)
    def _(li):
        acc[...] = jnp.zeros_like(acc)

        @pl.loop(0, CH)
        def _(c):
            s = li * CH + c
            slot = c % 2

            @pl.when((li == 0) | (c == 0))
            def _():
                weights_loaded(slot)

            @pl.when((li > 0) & (c < CH - 1))
            def _():
                load_weights(c + 1, (c + 1) % 2)

            @pl.when(li == 0)
            def _():
                @pl.loop(0, T // TB)
                def _(t):
                    rows = tokens(t, TB)
                    gate = dot(a[rows, :], wg[slot])
                    up = dot(a[rows, :], wu[slot])
                    dz = dot(dy[rows, :], wd[slot]).astype(bf16).astype(f32)
                    sig = jax.nn.sigmoid(gate)
                    act = gate * sig
                    z[rows, :] = (act * up).astype(bf16)
                    du[rows, :] = (dz * act).astype(bf16)
                    dg[rows, :] = (dz * (up * (sig + act * (1.0 - sig)))).astype(bf16)

                    @pl.when((t == 0) & (s == 0))
                    def _():
                        gather_last(CH + 1)

                    @pl.when((t == 3) & (s == 0))
                    def _():
                        gather_forward(CH + 2)
                        gather_own_gu(CH + 3)

                    @pl.when((t == 3) & (s == 2))
                    def _():
                        gather_last(CH + 3)

                    @pl.when((t == 2) & (s > 0))
                    def _():
                        scatter_sum(s - 1)

            @pl.when((li > 0) & (c == 0))
            def _():
                @pl.loop(0, TILES)
                def _(t):
                    first_grads(0, t, 0)

            @pl.when(li > 0)
            def _():
                scatter_sum(s - 1)

            @pl.when(s > 0)
            def _():
                for copy in sib_copies():
                    copy.wait_send()

            for m, grad in enumerate((dg, du)):

                @pl.loop(0, F // WB)
                def _(n):
                    cols = tokens(n, WB)
                    w = dot(at[...].reshape(D, T), grad[:, cols])
                    owng[m, :, :, cols] = w[:HD].reshape(4, RB, WB)
                    sibg[m, :, :, cols] = w[HD:].reshape(4, RB, WB).astype(bf16)

                scatter_sib(s, m)

            @pl.when(s > 0)
            def _():
                scatter_final(s - 1)

            scatter_near(s, 0)

            @pl.when(li > 0)
            def _():
                pltpu.make_async_copy(z_hbm.at[c], z, z_sem).wait()

            @pl.loop(0, F // WB)
            def _(n):
                w = dot(dyt[...], z[:, tokens(n, WB)])
                for i in range(WB // (2 * CB)):
                    lo, hi = w[:, 2 * CB * i : 2 * CB * i + CB], w[:, 2 * CB * i + CB : 2 * CB * (i + 1)]
                    q = n * (WB // (2 * CB)) + i
                    ownd[q] = jnp.where(k == 0, lo, hi)
                    sibd[q] = jnp.where(k == 0, hi, lo).astype(bf16)

            scatter_sib(s, 2)
            scatter_near(s, 1)

            @pl.when(s == CH - 1)
            def _():
                pltpu.make_async_copy(x_hbm.at[0], a, in_sem.at[0]).start()

            @pl.when((s >= CH - 1) & (s < STEPS - 1))
            def _():
                pltpu.make_async_copy(z_hbm.at[s - (CH - 1)], z, z_sem).start()

            @pl.when(s < CH - 1)
            def _():
                gather_done(CH + 1 + s)

            @pl.when(li == 0)
            def _():
                load_weights((CH + s + 1) % STEPS, (c + 1) % 2)

            @pl.when((li > 0) & (c < CH - 1))
            def _():
                weights_loaded((c + 1) % 2)

            @pl.when(s == 1)
            def _():
                gather_forward(CH + 3)

            @pl.loop(0, T // AB)
            def _(t):
                rows = tokens(t, AB)
                acc[:, rows] += dot_nt(wg[slot], dg[rows, :]) + dot_nt(wu[slot], du[rows, :])

                @pl.when((li > 0) & (c < CH - 1))
                def _():
                    for i in range(AB // VB):
                        first_grads(c + 1, t * (AB // VB) + i, (c + 1) % 2)

                @pl.when(t == 0)
                def _():
                    scatter_near(s, 2)

                @pl.when((t == 0) & (s == 0))
                def _():
                    gather_last(CH + 2)

        @pl.when(li == 0)
        def _():
            pltpu.make_async_copy(x_hbm.at[0], a, in_sem.at[0]).wait()

        @pl.loop(0, T // VB)
        def _(t):
            rows = tokens(t, VB)
            da = acc[:, rows].T.astype(bf16).astype(f32)
            wide = h[rows, :].astype(f32)
            scale = scale_of(wide)
            along = jnp.mean(da * wide, -1, keepdims=True)
            dwide = (da * scale - wide * (along * scale * scale * scale)).astype(bf16)
            v = (dy[rows, :].astype(f32) + dwide.astype(f32)).astype(bf16)
            dy[rows, :] = v

            @pl.when(li == 0)
            def _():
                dyt[:, rows] = v.T
                x = a[rows, :]
                h[rows, :] = x
                set_at(rows, x.astype(f32))

            @pl.when(li > 0)
            def _():
                pltpu.make_async_copy(dy.at[rows], dx_hbm.at[0, rows], in_sem.at[1]).start()

                @pl.when(t == 2)
                def _():
                    scatter_sum(STEPS - 1)

    last = STEPS - 1
    scatter_final(last)
    for copy in (*sib_copies(), *near_copies(0), *near_copies(1), *near_copies(2), *sum_copies()):
        copy.wait_send()
    out_stored()
    for copy in (*own_gu(last), *own_dn(last), *forward_gu(last), *forward_dn(last), *last_copies(last)):
        copy.wait_send()
    pltpu.make_async_copy(dy, dx_hbm.at[0], in_sem.at[1]).wait()


def pieces(refs):
    for ref in refs:
        if ref.shape[0] == 1:
            for i in range(4):
                yield ref.at[0, pl.ds(i * (T // 4), T // 4)]
        else:
            for i in range(LAYERS):
                yield ref.at[i]


def results(*refs):
    here, there, held = refs[:4], refs[4:8], refs[8:12]
    get, put = refs[12:]
    trips = list(zip(pieces(here), pieces(held), pieces(there), strict=True))
    for i, (src, mid, _) in enumerate(trips):
        pltpu.make_async_copy(src, mid, get.at[i]).start()
    for i, (src, mid, dst) in enumerate(trips):
        pltpu.make_async_copy(src, mid, get.at[i]).wait()
        pltpu.make_async_copy(mid, dst, put.at[i]).start()
    for i, (_, mid, dst) in enumerate(trips):
        pltpu.make_async_copy(mid, dst, put.at[i]).wait()


def on_device(x, dy, w_gate, w_up, w_down):
    hbm = pl.BlockSpec(memory_space=pl.ANY)
    shapes = (
        jax.ShapeDtypeStruct((1, T, D), bf16),
        jax.ShapeDtypeStruct((LAYERS, RB, FF), bf16),
        jax.ShapeDtypeStruct((LAYERS, RB, FF), bf16),
        jax.ShapeDtypeStruct((LAYERS, CH * CB, D), bf16),
        jax.ShapeDtypeStruct((STEPS, N, 2, RB, F), bf16),
        jax.ShapeDtypeStruct((STEPS, N, D, CB), bf16),
        jax.ShapeDtypeStruct((CH, TILES, 2, VB, F), f32),
        jax.ShapeDtypeStruct((CH, T, F), bf16),
    )
    act = pltpu.VMEM((T, D), bf16)
    wide = pltpu.VMEM((T, F), bf16)
    gu, down = pltpu.VMEM((2, RB, F), bf16), pltpu.VMEM((D, CB), bf16)
    dma = pltpu.SemaphoreType.DMA
    scratch = [
        *[pltpu.VMEM((2, D, F), bf16)] * 3,
        act, act, pltpu.VMEM((2, 4, RB, T), bf16), act, pltpu.VMEM((D, T), bf16),
        wide, wide, wide, pltpu.VMEM((D, T), f32),
        pltpu.VMEM((2, 4, RB, F), f32), pltpu.VMEM((4, D, CB), f32),
        *[pltpu.VMEM((2, 4, RB, F), bf16), pltpu.VMEM((4, D, CB), bf16)] * 2,
        *[gu, down] * 6,
        pltpu.VMEM((2, RB, F), f32), pltpu.VMEM((D, CB), f32), gu, pltpu.VMEM((CB, D), bf16),
        pltpu.VMEM((2, 2, RB, F), bf16), pltpu.VMEM((STEPS, D, CB), bf16), pltpu.VMEM((2, 2, VB, F), f32),
        dma((16,)), dma((STEPS, 16)), dma((2, 3)), dma((21,)), dma((21,)), dma((2,)), dma((4,)), dma((2,)), dma((2,)), dma,
        pltpu.SemaphoreType.REGULAR, pltpu.SemaphoreType.REGULAR((2,)), pltpu.SemaphoreType.REGULAR((2,)),
    ]
    grads = pl.pallas_call(
        kernel,
        out_shape=shapes,
        in_specs=[hbm] * 5,
        out_specs=[hbm] * 8,
        scratch_shapes=scratch,
        compiler_params=pltpu.CompilerParams(collective_id=0, has_side_effects=True, vmem_limit_bytes=67_000_000),
        name="layers",
    )(x, dy, w_gate, w_up, w_down)[:4]
    return pl.pallas_call(
        results,
        out_shape=shapes[:4],
        in_specs=[hbm] * 4,
        out_specs=[hbm] * 4,
        scratch_shapes=[pltpu.VMEM(s.shape, bf16) for s in shapes[:4]] + [dma((PIECES,)), dma((PIECES,))],
        compiler_params=pltpu.CompilerParams(vmem_limit_bytes=67_000_000),
        name="results",
    )(*grads)


def solution(mesh):
    act, weight = P(("rep", "dp")), P(None, "dp")
    grad = P("rep", "dp")
    return jax.shard_map(
        on_device,
        mesh=mesh,
        in_specs=(act, act, weight, weight, weight),
        out_specs=(act, grad, grad, grad),
        check_vma=False,
    )
```

```python
import jax
import jax.numpy as jnp
from jax import lax
from jax.experimental import pallas as pl
from jax.experimental.pallas import tpu as pltpu
from jax.sharding import PartitionSpec as P

N = 8
T, D, FF, LAYERS = 2048, 640, 4096, 2
CH = 4
F = FF // CH
RB = D // N
CB = F // N
HD = D // 2
STEPS = LAYERS * CH
TB = 512
VB = 256
WB = 1024
PIECES = 4 + 3 * LAYERS
AB = 1024
TILES = T // VB

f32, bf16 = jnp.float32, jnp.bfloat16


def dot(a, b):
    return jnp.dot(a, b, preferred_element_type=f32)


def dot_nt(a, b):
    return lax.dot_general(a, b, (((1,), (1,)), ((), ())), preferred_element_type=f32)


def kernel(
    x_hbm, dy_hbm, wg_hbm, wu_hbm, wd_hbm,
    dx_hbm, outg_hbm, outu_hbm, outd_hbm, gu_all, dn_all, saved_hbm, z_hbm,
    wg, wu, wd, h, a, at, dy, dyt, z, dg, du, acc,
    owng, ownd, sibg, sibd, recg, recd, sdg, sdd, rdg, rdd,
    sxg, sxd, syg, syd, bxg, bxd, byg, byd, fing, find, og, od,
    packed, dn_own, saved,
    ag_send, ag_recv, load_sem, rs_send, rs_recv, out_sem, in_sem, pack_sem, saved_sem, z_sem, free_sib, free_diag, free_block,
):
    me = lax.axis_index("dp")
    k = me % 2
    cy = (me // 2) % 2
    cx = me // 4
    chip = 2 * cx + cy
    sib = 2 * chip + (1 - k)
    chip_x = 2 * (1 - cx) + cy
    chip_y = 2 * cx + (1 - cy)
    chip_d = 2 * (1 - cx) + (1 - cy)
    xn, yn, dn = 2 * chip_x + k, 2 * chip_y + k, 2 * chip_d + k

    def far(src, dst, ss, rs, to):
        return pltpu.make_async_remote_copy(
            src_ref=src, dst_ref=dst, send_sem=ss, recv_sem=rs, device_id={"dp": to}, device_id_type=pl.DeviceIdType.MESH
        )

    def signal(sem, to):
        pl.semaphore_signal(sem, inc=1, device_id={"dp": to}, device_id_type=pl.DeviceIdType.MESH)

    def own_gu(j):
        for i, to in enumerate((xn, yn, sib)):
            yield far(packed.at[j % 2], gu_all.at[j, me], ag_send.at[2 * i], ag_recv.at[j, (0, 2, 8)[i]], to)

    def own_dn(j):
        for i, to in enumerate((xn, yn, sib)):
            yield far(dn_own.at[j], dn_all.at[j, me], ag_send.at[2 * i + 1], ag_recv.at[j, (1, 3, 9)[i]], to)

    def slabs(j):
        layer, c = j // CH, j % CH
        for d in range(N):
            yield layer, pl.ds(pl.multiple_of(CH * CB * d + CB * c, CB), CB), pl.ds(CB * d, CB)

    def pack(j):
        for layer, there, here in slabs(j):
            for m, w in enumerate((wg_hbm, wu_hbm)):
                pltpu.make_async_copy(w.at[layer, :, there], packed.at[j % 2, m, :, here], pack_sem.at[j % 2]).start()

    def forward_gu(j):
        yield far(gu_all.at[j, xn, 0], gu_all.at[j, xn, 0], ag_send.at[6], ag_recv.at[j, 4], yn)
        yield far(gu_all.at[j, yn, 1], gu_all.at[j, yn, 1], ag_send.at[8], ag_recv.at[j, 6], xn)
        for i, src in enumerate((xn, yn)):
            yield far(gu_all.at[j, src], gu_all.at[j, src], ag_send.at[10 + 2 * i], ag_recv.at[j, 10 + 2 * i], sib)

    def forward_dn(j):
        top, bot = pl.ds(0, HD), pl.ds(HD, HD)
        yield far(dn_all.at[j, xn, top], dn_all.at[j, xn, top], ag_send.at[7], ag_recv.at[j, 5], yn)
        yield far(dn_all.at[j, yn, bot], dn_all.at[j, yn, bot], ag_send.at[9], ag_recv.at[j, 7], xn)
        for i, src in enumerate((xn, yn)):
            yield far(dn_all.at[j, src], dn_all.at[j, src], ag_send.at[11 + 2 * i], ag_recv.at[j, 11 + 2 * i], sib)

    def last_copies(j):
        yield far(gu_all.at[j, dn], gu_all.at[j, dn], ag_send.at[14], ag_recv.at[j, 14], sib)
        yield far(dn_all.at[j, dn], dn_all.at[j, dn], ag_send.at[15], ag_recv.at[j, 15], sib)

    def arrived(ref, j, r, frm):
        far(ref, ref, ag_send.at[0], ag_recv.at[j, r], frm).wait_recv()

    def gather_own_dn(j):
        @pl.when(j > 0)
        def _():
            for copy in own_dn(j):
                copy.wait_send()

        for copy in own_dn(j):
            copy.start()

    def gather_own_gu(j):
        pltpu.make_async_copy(packed.at[j % 2], packed.at[j % 2], pack_sem.at[j % 2]).wait()

        @pl.when(j > 0)
        def _():
            for copy in own_gu(j):
                copy.wait_send()

        for copy in own_gu(j):
            copy.start()

        @pl.when((j > 0) & (j < STEPS - 1))
        def _():
            pack(j + 1)

    def gather_forward_gu(j):
        arrived(gu_all.at[j, xn], j, 0, xn)
        arrived(gu_all.at[j, yn], j, 2, yn)

        @pl.when(j > 0)
        def _():
            for copy in forward_gu(j):
                copy.wait_send()

        for copy in forward_gu(j):
            copy.start()

    def gather_forward_dn(j):
        arrived(dn_all.at[j, xn], j, 1, xn)
        arrived(dn_all.at[j, yn], j, 3, yn)

        @pl.when(j > 0)
        def _():
            for copy in forward_dn(j):
                copy.wait_send()

        for copy in forward_dn(j):
            copy.start()

    def gather_forward(j):
        gather_forward_dn(j)
        gather_forward_gu(j)

    def gather_last(j):
        top, bot = pl.ds(0, HD), pl.ds(HD, HD)
        arrived(gu_all.at[j, dn, 0], j, 4, yn)
        arrived(dn_all.at[j, dn, top], j, 5, yn)
        arrived(gu_all.at[j, dn, 1], j, 6, xn)
        arrived(dn_all.at[j, dn, bot], j, 7, xn)

        @pl.when(j > 0)
        def _():
            for copy in last_copies(j):
                copy.wait_send()

        for copy in last_copies(j):
            copy.start()

    def gather_sib(j, which):
        for i in which:
            src = 2 * (chip, chip_x, chip_y, chip_d)[i] + (1 - k)
            arrived(gu_all.at[j, src], j, 8 + 2 * i, sib)
            arrived(dn_all.at[j, src], j, 9 + 2 * i, sib)

    def gather_done(j):
        gather_sib(j, range(4))

    def load_pieces(j, slot, sources, own=False):
        def rows(src):
            return pl.ds(pl.multiple_of(src * RB, RB), RB)

        def cols(src):
            return pl.ds(pl.multiple_of(src * CB, CB), CB)

        for src in sources:
            pltpu.make_async_copy(gu_all.at[j, src, 0], wg.at[slot, rows(src)], load_sem.at[slot, 0]).start()
            pltpu.make_async_copy(gu_all.at[j, src, 1], wu.at[slot, rows(src)], load_sem.at[slot, 1]).start()
            pltpu.make_async_copy(dn_all.at[j, src], wd.at[slot, :, cols(src)], load_sem.at[slot, 2]).start()
        if own:
            for layer, there, here in slabs(j):
                for m, (w, to) in enumerate(((wg_hbm, wg), (wu_hbm, wu))):
                    pltpu.make_async_copy(w.at[layer, :, there], to.at[slot, rows(me), here], load_sem.at[slot, m]).start()
            pltpu.make_async_copy(dn_own.at[j], wd.at[slot, :, cols(me)], load_sem.at[slot, 2]).start()

    def load_weights(j, slot):
        load_pieces(j, slot, [(me + i) % N for i in range(1, N)], own=True)

    def weights_loaded(slot):
        for i, w in enumerate((wg, wu, wd)):
            pltpu.make_async_copy(w.at[slot], w.at[slot], load_sem.at[slot, i]).wait()

    def sib_copies():
        return (
            far(sibg.at[0], recg.at[0], rs_send.at[0], rs_recv.at[0], sib),
            far(sibg.at[1], recg.at[1], rs_send.at[1], rs_recv.at[1], sib),
            far(sibd, recd, rs_send.at[2], rs_recv.at[2], sib),
        )

    def halves(which):
        if which == 2:
            return lambda g, d: (d.at[pl.ds(0, HD)], d.at[pl.ds(HD, HD)])
        return lambda g, d: (g.at[which, :, pl.ds(0, F // 2)], g.at[which, :, pl.ds(F // 2, F // 2)])

    def near_copies(which):
        of, i = halves(which), 3 + 4 * which
        return (
            far(of(sdg, sdd)[0], of(rdg, rdd)[0], rs_send.at[i], rs_recv.at[i], xn),
            far(of(sdg, sdd)[1], of(rdg, rdd)[1], rs_send.at[i + 1], rs_recv.at[i + 1], yn),
            far(of(sxg, sxd)[0], of(bxg, bxd)[0], rs_send.at[i + 2], rs_recv.at[i + 2], xn),
            far(of(syg, syd)[1], of(byg, byd)[1], rs_send.at[i + 3], rs_recv.at[i + 3], yn),
        )

    def sum_copies():
        copies = []
        for which in range(3):
            of, i = halves(which), 15 + 2 * which
            copies.append(far(of(sxg, sxd)[1], of(bxg, bxd)[1], rs_send.at[i], rs_recv.at[i], xn))
            copies.append(far(of(syg, syd)[0], of(byg, byd)[0], rs_send.at[i + 1], rs_recv.at[i + 1], yn))
        return copies

    def diag_arrived():
        for which in range(3):
            for copy in near_copies(which)[:2]:
                copy.wait_recv()

    def blocks_arrived():
        for which in range(3):
            for copy in near_copies(which)[2:]:
                copy.wait_recv()
        for copy in sum_copies():
            copy.wait_recv()

    def store_out(j):
        for layer, there, here in slabs(j):
            for m, out in enumerate((outg_hbm, outu_hbm)):
                pltpu.make_async_copy(og.at[m, :, here], out.at[layer, :, there], out_sem.at[0]).start()
        rows = pl.ds(pl.multiple_of(j % CH * CB, CB), CB)
        pltpu.make_async_copy(od, outd_hbm.at[j // CH, rows], out_sem.at[1]).start()

    def out_stored():
        pltpu.make_async_copy(og, og, out_sem.at[0]).wait()
        pltpu.make_async_copy(od, od, out_sem.at[1]).wait()

    def scatter_sib(s, which):
        if which == 0:
            @pl.when(s > 0)
            def _():
                pl.semaphore_wait(free_sib, 1)

        sib_copies()[which].start()

    def scatter_near(s, which):
        @pl.when(s > 0)
        def _():
            for copy in near_copies(which):
                copy.wait_send()

        sib_copies()[which].wait_recv()
        top, bot = pl.ds(0, HD), pl.ds(HD, HD)
        if which < 2:
            m = which
            fing[m] = owng[m, chip] + recg[m, chip].astype(f32)
            sdg[m] = (owng[m, chip_d] + recg[m, chip_d].astype(f32)).astype(bf16)
            far_x = owng[m, chip_x] + recg[m, chip_x].astype(f32)
            far_y = owng[m, chip_y] + recg[m, chip_y].astype(f32)
            sxg[m, :, : F // 2] = far_x[:, : F // 2].astype(bf16)
            owng[m, chip_x, :, F // 2 :] = far_x[:, F // 2 :]
            syg[m, :, F // 2 :] = far_y[:, F // 2 :].astype(bf16)
            owng[m, chip_y, :, : F // 2] = far_y[:, : F // 2]

            if m == 0:
                @pl.when(s > 0)
                def _():
                    for sem in (free_diag, free_block):
                        for i in range(2):
                            pl.semaphore_wait(sem.at[i], 1)
        else:
            find[...] = ownd[chip] + recd[chip].astype(f32)
            sdd[...] = (ownd[chip_d] + recd[chip_d].astype(f32)).astype(bf16)
            sxd[top] = (ownd[chip_x, top] + recd[chip_x, top].astype(f32)).astype(bf16)
            ownd[chip_x, bot] = ownd[chip_x, bot] + recd[chip_x, bot].astype(f32)
            syd[bot] = (ownd[chip_y, bot] + recd[chip_y, bot].astype(f32)).astype(bf16)
            ownd[chip_y, top] = ownd[chip_y, top] + recd[chip_y, top].astype(f32)

            @pl.when(s < STEPS - 1)
            def _():
                signal(free_sib, sib)

        for copy in near_copies(which):
            copy.start()

    def scatter_sum(s):
        @pl.when(s > 0)
        def _():
            for copy in sum_copies():
                copy.wait_send()

        diag_arrived()
        top, bot = pl.ds(0, HD), pl.ds(HD, HD)
        lo, hi = pl.ds(0, F // 2), pl.ds(F // 2, F // 2)
        for m in range(2):
            sxg[m, :, hi] = (owng[m, chip_x, :, hi] + rdg[m, :, hi].astype(f32)).astype(bf16)
            syg[m, :, lo] = (owng[m, chip_y, :, lo] + rdg[m, :, lo].astype(f32)).astype(bf16)
        sxd[bot] = (ownd[chip_x, bot] + rdd[bot].astype(f32)).astype(bf16)
        syd[top] = (ownd[chip_y, top] + rdd[top].astype(f32)).astype(bf16)

        @pl.when(s < STEPS - 1)
        def _():
            signal(free_diag.at[0], xn)
            signal(free_diag.at[1], yn)

        for copy in sum_copies():
            copy.start()

    def scatter_final(s):
        j = CH * (1 - s // CH) + s % CH

        @pl.when(s > 0)
        def _():
            out_stored()

        blocks_arrived()
        for m in range(2):
            og[m] = (fing[m] + bxg[m].astype(f32) + byg[m].astype(f32)).astype(bf16)
        od[...] = (find[...] + bxd[...].astype(f32) + byd[...].astype(f32)).T.astype(bf16)

        @pl.when(s < STEPS - 1)
        def _():
            signal(free_block.at[0], xn)
            signal(free_block.at[1], yn)

        store_out(j)

    def scale_of(wide):
        return lax.rsqrt(jnp.mean(wide * wide, -1, keepdims=True) + 1e-6)

    def tokens(t, n):
        return pl.ds(pl.multiple_of(t * n, n), n)

    def store_at(rows, v):
        vt = v.T
        for d in range(N):
            at[(d % 2 + k) % 2, d // 2, :, rows] = vt[d * RB : (d + 1) * RB]

    def set_at(rows, wide):
        store_at(rows, (wide * scale_of(wide)).astype(bf16))

    def set_a(rows, wide):
        v = (wide * scale_of(wide)).astype(bf16)
        a[rows, :] = v
        store_at(rows, v)

    def store_saved(c, t):
        return pltpu.make_async_copy(saved.at[t % 2], saved_hbm.at[c, t], saved_sem.at[t % 2])

    def load_saved(n):
        return pltpu.make_async_copy(saved_hbm.at[n // TILES, n % TILES], saved.at[n % 2], saved_sem.at[n % 2])

    pack(0)
    pack(1)
    raw = a.at[pl.ds(0, LAYERS * CH * CB)]
    load_dn = [pltpu.make_async_copy(wd_hbm.at[i], raw.at[pl.ds(i * CH * CB, CH * CB)], in_sem.at[2 + i]) for i in range(LAYERS)]
    load_x = pltpu.make_async_copy(x_hbm.at[0], h, in_sem.at[0])
    load_dy = pltpu.make_async_copy(dy_hbm.at[0], dy, in_sem.at[1])
    for copy in (*load_dn, load_x, load_dy):
        copy.start()
    barrier = pltpu.get_barrier_semaphore()
    for to in (sib, xn, yn):
        signal(barrier, to)
    pl.semaphore_wait(barrier, 3)

    gather_own_gu(0)
    for copy in load_dn:
        copy.wait()

    @pl.loop(0, STEPS)
    def _(j):
        dn_own[j] = a[tokens(j, CB), :].T

    gather_own_dn(0)
    gather_own_dn(1)
    load_x.wait()
    load_dy.wait()
    acc[...] = jnp.zeros_like(acc)

    @pl.loop(0, T // VB)
    def _(t):
        rows = tokens(t, VB)
        set_a(rows, h[rows, :].astype(f32))
        dyt[:, rows] = dy[rows, :].T

    gather_forward_gu(0)
    gather_forward_dn(0)
    gather_own_gu(1)
    gather_own_dn(2)
    gather_last(0)
    gather_done(0)
    load_weights(0, 0)

    @pl.loop(0, CH)
    def _(c):
        slot = c % 2
        weights_loaded(slot)

        @pl.when(c > 0)
        def _():
            pltpu.make_async_copy(z, z_hbm.at[c], z_sem).wait()

        @pl.loop(0, TILES)
        def _(t):
            rows = tokens(t, VB)

            @pl.when(c * TILES + t > 1)
            def _():
                store_saved(c, t).wait()

            gate = dot(a[rows, :], wg[slot])
            up = dot(a[rows, :], wu[slot])
            sig = jax.nn.sigmoid(gate)
            act = gate * sig
            z[rows, :] = (act * up).astype(bf16)
            saved[t % 2, 0] = act
            saved[t % 2, 1] = up * (sig + act * (1.0 - sig))
            store_saved(c, t).start()

            @pl.when(t == 1)
            def _():
                gather_forward(c + 1)
                gather_own_gu(c + 2)
                load_pieces(c + 1, (c + 1) % 2, (xn, yn), own=True)

            @pl.when(t == TILES - 2)
            def _():
                gather_sib(c + 1, range(3))
                load_pieces(c + 1, (c + 1) % 2, [2 * q + (1 - k) for q in (chip, chip_x, chip_y)])

        pltpu.make_async_copy(z, z_hbm.at[c], z_sem).start()

        @pl.loop(0, T // AB)
        def _(t):
            rows = tokens(t, AB)
            acc[:, rows] += dot_nt(wd[slot], z[rows, :])

        gather_last(c + 1)
        gather_own_dn(c + 3)
        load_pieces(c + 1, (c + 1) % 2, (dn,))

        @pl.when(c < CH - 1)
        def _():
            gather_sib(c + 1, (3,))
            load_pieces(c + 1, (c + 1) % 2, (2 * chip_d + (1 - k),))

    @pl.loop(0, T // VB)
    def _(t):
        rows = tokens(t, VB)
        y = acc[:, rows].T.astype(bf16)
        v = (h[rows, :].astype(f32) + y.astype(f32)).astype(bf16)
        h[rows, :] = v
        set_a(rows, v.astype(f32))

        @pl.when(t == 4)
        def _():
            gather_sib(CH, (3,))
            load_pieces(CH, 0, (2 * chip_d + (1 - k),))

    gather_forward(CH + 1)
    gather_own_gu(CH + 2)
    gather_own_dn(CH + 3)

    pltpu.make_async_copy(z, z_hbm.at[CH - 1], z_sem).wait()
    for t in (0, 1):
        store_saved(CH - 1, t).wait()
    for t in (0, 1):
        load_saved(t).start()

    def first_grads(c, t, slot):
        rows = tokens(t, VB)
        n = c * TILES + t
        dz = dot(dy[rows, :], wd[slot]).astype(bf16).astype(f32)
        load_saved(n).wait()
        du[rows, :] = (dz * saved[n % 2, 0]).astype(bf16)
        dg[rows, :] = (dz * saved[n % 2, 1]).astype(bf16)

        @pl.when(n < CH * TILES - 2)
        def _():
            load_saved(n + 2).start()

    @pl.loop(0, LAYERS)
    def _(li):
        acc[...] = jnp.zeros_like(acc)

        @pl.loop(0, CH)
        def _(c):
            s = li * CH + c
            slot = c % 2

            @pl.when((li == 0) | (c == 0))
            def _():
                weights_loaded(slot)

            @pl.when((li > 0) & (c < CH - 1))
            def _():
                load_weights(c + 1, (c + 1) % 2)

            @pl.when(li == 0)
            def _():
                @pl.loop(0, T // TB)
                def _(t):
                    rows = tokens(t, TB)
                    gate = dot(a[rows, :], wg[slot])
                    up = dot(a[rows, :], wu[slot])
                    dz = dot(dy[rows, :], wd[slot]).astype(bf16).astype(f32)
                    sig = jax.nn.sigmoid(gate)
                    act = gate * sig
                    z[rows, :] = (act * up).astype(bf16)
                    du[rows, :] = (dz * act).astype(bf16)
                    dg[rows, :] = (dz * (up * (sig + act * (1.0 - sig)))).astype(bf16)

                    @pl.when((t == 0) & (s == 0))
                    def _():
                        gather_last(CH + 1)

                    @pl.when((t == 3) & (s == 0))
                    def _():
                        gather_forward(CH + 2)
                        gather_own_gu(CH + 3)

                    @pl.when((t == 3) & (s == 2))
                    def _():
                        gather_last(CH + 3)

                    @pl.when((t == 2) & (s > 0))
                    def _():
                        scatter_sum(s - 1)

            @pl.when((li > 0) & (c == 0))
            def _():
                @pl.loop(0, TILES)
                def _(t):
                    first_grads(0, t, 0)

            @pl.when(li > 0)
            def _():
                scatter_sum(s - 1)

            @pl.when(s > 0)
            def _():
                for copy in sib_copies():
                    copy.wait_send()

            for m, grad in enumerate((dg, du)):

                @pl.loop(0, F // WB)
                def _(n):
                    cols = tokens(n, WB)
                    w = dot(at[...].reshape(D, T), grad[:, cols])
                    owng[m, :, :, cols] = w[:HD].reshape(4, RB, WB)
                    sibg[m, :, :, cols] = w[HD:].reshape(4, RB, WB).astype(bf16)

                scatter_sib(s, m)

            @pl.when(s > 0)
            def _():
                scatter_final(s - 1)

            scatter_near(s, 0)

            @pl.when(li > 0)
            def _():
                pltpu.make_async_copy(z_hbm.at[c], z, z_sem).wait()

            @pl.loop(0, F // WB)
            def _(n):
                w = dot(dyt[...], z[:, tokens(n, WB)])
                for i in range(WB // (2 * CB)):
                    lo, hi = w[:, 2 * CB * i : 2 * CB * i + CB], w[:, 2 * CB * i + CB : 2 * CB * (i + 1)]
                    q = n * (WB // (2 * CB)) + i
                    ownd[q] = jnp.where(k == 0, lo, hi)
                    sibd[q] = jnp.where(k == 0, hi, lo).astype(bf16)

            scatter_sib(s, 2)
            scatter_near(s, 1)

            @pl.when(s == CH - 1)
            def _():
                pltpu.make_async_copy(x_hbm.at[0], a, in_sem.at[0]).start()

            @pl.when((s >= CH - 1) & (s < STEPS - 1))
            def _():
                pltpu.make_async_copy(z_hbm.at[s - (CH - 1)], z, z_sem).start()

            @pl.when(s < CH - 1)
            def _():
                gather_done(CH + 1 + s)

            @pl.when(li == 0)
            def _():
                load_weights((CH + s + 1) % STEPS, (c + 1) % 2)

            @pl.when((li > 0) & (c < CH - 1))
            def _():
                weights_loaded((c + 1) % 2)

            @pl.when(s == 1)
            def _():
                gather_forward(CH + 3)

            @pl.loop(0, T // AB)
            def _(t):
                rows = tokens(t, AB)
                acc[:, rows] += dot_nt(wg[slot], dg[rows, :]) + dot_nt(wu[slot], du[rows, :])

                @pl.when((li > 0) & (c < CH - 1))
                def _():
                    for i in range(AB // VB):
                        first_grads(c + 1, t * (AB // VB) + i, (c + 1) % 2)

                @pl.when(t == 0)
                def _():
                    scatter_near(s, 2)

                @pl.when((t == 0) & (s == 0))
                def _():
                    gather_last(CH + 2)

        @pl.when(li == 0)
        def _():
            pltpu.make_async_copy(x_hbm.at[0], a, in_sem.at[0]).wait()

        @pl.loop(0, T // TB)
        def _(t):
            rows = tokens(t, TB)
            da = acc[:, rows].T.astype(bf16).astype(f32)
            wide = h[rows, :].astype(f32)
            scale = scale_of(wide)
            along = jnp.mean(da * wide, -1, keepdims=True)
            dwide = (da * scale - wide * (along * scale * scale * scale)).astype(bf16)
            v = (dy[rows, :].astype(f32) + dwide.astype(f32)).astype(bf16)
            dy[rows, :] = v

            @pl.when(li == 0)
            def _():
                dyt[:, rows] = v.T
                x = a[rows, :]
                h[rows, :] = x
                set_at(rows, x.astype(f32))

            @pl.when(li > 0)
            def _():
                pltpu.make_async_copy(dy.at[rows], dx_hbm.at[0, rows], in_sem.at[1]).start()

                @pl.when(t == 1)
                def _():
                    scatter_sum(STEPS - 1)

    last = STEPS - 1
    scatter_final(last)
    for copy in (*sib_copies(), *near_copies(0), *near_copies(1), *near_copies(2), *sum_copies()):
        copy.wait_send()
    out_stored()
    for copy in (*own_gu(last), *own_dn(last), *forward_gu(last), *forward_dn(last), *last_copies(last)):
        copy.wait_send()
    pltpu.make_async_copy(dy, dx_hbm.at[0], in_sem.at[1]).wait()


def pieces(refs):
    for ref in refs:
        if ref.shape[0] == 1:
            for i in range(4):
                yield ref.at[0, pl.ds(i * (T // 4), T // 4)]
        else:
            for i in range(LAYERS):
                yield ref.at[i]


def results(*refs):
    here, there, held = refs[:4], refs[4:8], refs[8:12]
    get, put = refs[12:]
    trips = list(zip(pieces(here), pieces(held), pieces(there), strict=True))
    for i, (src, mid, _) in enumerate(trips):
        pltpu.make_async_copy(src, mid, get.at[i]).start()
    for i, (src, mid, dst) in enumerate(trips):
        pltpu.make_async_copy(src, mid, get.at[i]).wait()
        pltpu.make_async_copy(mid, dst, put.at[i]).start()
    for i, (_, mid, dst) in enumerate(trips):
        pltpu.make_async_copy(mid, dst, put.at[i]).wait()


def on_device(x, dy, w_gate, w_up, w_down):
    hbm = pl.BlockSpec(memory_space=pl.ANY)
    shapes = (
        jax.ShapeDtypeStruct((1, T, D), bf16),
        jax.ShapeDtypeStruct((LAYERS, RB, FF), bf16),
        jax.ShapeDtypeStruct((LAYERS, RB, FF), bf16),
        jax.ShapeDtypeStruct((LAYERS, CH * CB, D), bf16),
        jax.ShapeDtypeStruct((STEPS, N, 2, RB, F), bf16),
        jax.ShapeDtypeStruct((STEPS, N, D, CB), bf16),
        jax.ShapeDtypeStruct((CH, TILES, 2, VB, F), f32),
        jax.ShapeDtypeStruct((CH, T, F), bf16),
    )
    act = pltpu.VMEM((T, D), bf16)
    wide = pltpu.VMEM((T, F), bf16)
    gu, down = pltpu.VMEM((2, RB, F), bf16), pltpu.VMEM((D, CB), bf16)
    dma = pltpu.SemaphoreType.DMA
    scratch = [
        *[pltpu.VMEM((2, D, F), bf16)] * 3,
        act, act, pltpu.VMEM((2, 4, RB, T), bf16), act, pltpu.VMEM((D, T), bf16),
        wide, wide, wide, pltpu.VMEM((D, T), f32),
        pltpu.VMEM((2, 4, RB, F), f32), pltpu.VMEM((4, D, CB), f32),
        *[pltpu.VMEM((2, 4, RB, F), bf16), pltpu.VMEM((4, D, CB), bf16)] * 2,
        *[gu, down] * 6,
        pltpu.VMEM((2, RB, F), f32), pltpu.VMEM((D, CB), f32), gu, pltpu.VMEM((CB, D), bf16),
        pltpu.VMEM((2, 2, RB, F), bf16), pltpu.VMEM((STEPS, D, CB), bf16), pltpu.VMEM((2, 2, VB, F), f32),
        dma((16,)), dma((STEPS, 16)), dma((2, 3)), dma((21,)), dma((21,)), dma((2,)), dma((4,)), dma((2,)), dma((2,)), dma,
        pltpu.SemaphoreType.REGULAR, pltpu.SemaphoreType.REGULAR((2,)), pltpu.SemaphoreType.REGULAR((2,)),
    ]
    grads = pl.pallas_call(
        kernel,
        out_shape=shapes,
        in_specs=[hbm] * 5,
        out_specs=[hbm] * 8,
        scratch_shapes=scratch,
        compiler_params=pltpu.CompilerParams(collective_id=0, has_side_effects=True, vmem_limit_bytes=67_000_000),
        name="layers",
    )(x, dy, w_gate, w_up, w_down)[:4]
    return pl.pallas_call(
        results,
        out_shape=shapes[:4],
        in_specs=[hbm] * 4,
        out_specs=[hbm] * 4,
        scratch_shapes=[pltpu.VMEM(s.shape, bf16) for s in shapes[:4]] + [dma((PIECES,)), dma((PIECES,))],
        compiler_params=pltpu.CompilerParams(vmem_limit_bytes=67_000_000),
        name="results",
    )(*grads)


def solution(mesh):
    act, weight = P(("rep", "dp")), P(None, "dp")
    grad = P("rep", "dp")
    return jax.shard_map(
        on_device,
        mesh=mesh,
        in_specs=(act, act, weight, weight, weight),
        out_specs=(act, grad, grad, grad),
        check_vma=False,
    )
```
